32 devices in a mesh: batch: 2 (over core), expert: 4 (over y, x), dim: 4 (over z).
Axes of the slice: x: 2, y: 2, z: 4, core: 2. Of those that a mesh axis runs over, the one named last changes fastest.
Arguments:
- inputs: bfloat16 [2048, 4096], P('batch', 'dim'), may hold values from -6 to 6
- expert_ids: int32 [2048, 4], P('batch'), may hold values from 0 to 7, all different within a row; in each aligned block of 1024 rows (0 to 1023, 1024 to 2047, ...) at most 1024 rows name the same one
- gate_weight: bfloat16 [4096, 8], P('dim'), may hold values from -0.09375 to 0.09375
- reduce_weight: bfloat16 [8, 4096, 256], P('expert', ('dim', 'batch')), may hold values from -0.09375 to 0.09375
- middle_weight: bfloat16 [8, 256, 256], P('expert', 'batch'), may hold values from -0.375 to 0.375
- expand_weight: bfloat16 [8, 4096, 256], P('expert', ('dim', 'batch')), may hold values from -0.375 to 0.375
- bias: float32 [4096], P('dim'), may hold values from -3 to 3
Outputs:
- crossed: bfloat16 [2048, 4096], P(('batch', 'expert'), 'dim')
The draws below stay inside these ranges and needn't reach their ends.
Inputs may be any that keep to these rules, and one draw needn't show every extreme that they name: `expert_ids`: each row names 4 different experts; in each aligned block of 1024 rows (the examples of one index of batch) no expert is named by more than 1024 rows, and in some block one expert is named by exactly 1024 rows.
All inputs are finite; a program needn't handle non-finite values.
Results may differ from the reference program's by a relative error of at most 0.012.
Values may be sent and summed in bfloat16 or wider, within the bound.
No kernel may reach another device: no remote copies, remote signals or barrier semaphores. Data moves between devices by JAX's collectives and lax.ppermute only.
A program may use at most 64 MiB of HBM per device.

```python
import math
import jax
import jax.numpy as jnp
import numpy as np
from jax import lax

D = 4096
RANK = 256
EXPERTS = 8
TOP = 4
TOK_DEV = 1024
CAP = 1024
TOKENS = 2048
N_BATCH = 2
N_EXPERT = 4


def shard_levels(own_key, shape, pieces, smallest, largest):
    def one(dim, parts):
        steps = jax.random.uniform(jax.random.fold_in(jax.random.fold_in(own_key, 6), dim), (parts,), jnp.float32, smallest / len(pieces), largest / len(pieces))
        return jnp.repeat(jnp.exp(steps), shape[dim] // parts).reshape((-1,) + (1,) * (len(shape) - dim - 1))

    factor_of = one(*pieces[0])
    for cut in pieces[1:]:
        factor_of = factor_of * one(*cut)
    return factor_of


def assign_block(own_key, own, number, rows, amount, top, reach, skew):
    order = jax.random.permutation(own_key, amount)
    packed, ordinary = load_shares(amount, rows * top, reach, skew, True), load_shares(amount, rows * top, reach, skew, False)
    places = jnp.arange(amount)

    def named(sizes, rotation):
        used = int((sizes > 0).sum())
        fixed = max(1, used // 4)
        passed = fixed + (places - fixed + rotation * (used - fixed)) % max(1, amount - fixed)
        return jnp.zeros((amount,), jnp.int32).at[order[jnp.where(places < fixed, places, passed)]].set(jnp.asarray(sizes, jnp.int32))

    sizes = jnp.where(number % 4 == 0, named(packed, number // 4), named(ordinary, number - number // 4 - 1))
    mixed = jax.random.permutation(jax.random.fold_in(own, 3), amount)
    giver, sink = mixed[0:amount // 2 * 2:2], mixed[1:amount // 2 * 2:2]
    margin = jnp.minimum(sizes[giver] - 1, reach - sizes[sink]) // 2
    margin = jnp.where((giver == order[0]) | (sink == order[0]) | (sizes[sink] == 0), 0, jnp.maximum(margin, 0))
    passed = jax.random.randint(jax.random.fold_in(own, 4), (amount // 2,), 0, 1 << 20) % (margin + 1)
    sizes = sizes.at[giver].add(-passed).at[sink].add(passed)
    labels = jnp.searchsorted(jnp.cumsum(sizes), jnp.arange(rows * top), side="right").astype(jnp.int32)
    listing = labels.reshape(top, rows).T
    listing = listing[jax.random.permutation(jax.random.fold_in(own, 1), rows)]
    rotation = jax.random.randint(jax.random.fold_in(own, 2), (rows, 1), 0, top)
    return jnp.take_along_axis(listing, (jnp.arange(top)[None, :] + rotation) % top, axis=1)


def load_shares(amount, total, reach, skew, full):
    portions = [(1 << 20) // math.isqrt(standing ** skew) + 1 for standing in range(1, amount + 1)]
    largest = reach if full else min(reach, max(-(-total // amount), total * portions[0] // sum(portions)))
    least = 1 if total - largest >= amount - 1 else 0
    counts, spare = [largest] + [least] * (amount - 1), total - largest - least * (amount - 1)
    while spare > 0:
        movable = [i for i in range(1, amount) if counts[i] < largest] or [i for i in range(1, amount) if counts[i] < reach]
        whole, remaining = sum([portions[i] for i in movable]), spare
        for i in movable:
            addition = min(reach - counts[i], max(1, remaining * portions[i] // whole), spare)
            counts[i] = counts[i] + addition
            spare = spare - addition
    return np.array(counts)


def bell_draw(own_key, extent, scale, limit, shards=(), kind=jnp.bfloat16):
    factor_of = shard_levels(own_key, extent, shards, -0.22, 0.18) if shards else 1.0
    entries = jax.random.normal(own_key, extent, jnp.float32) * scale * factor_of
    return jnp.minimum(jnp.maximum(entries, -limit), limit).astype(kind)


def setup_inputs(seed: int = 0) -> dict:
    key_list = jax.random.split(jax.random.key(seed), 8)
    inputs = bell_draw(key_list[0], (TOKENS, D), 1.0, 6.0, ((0, 2), (1, 4)))
    expert_ids_keys = jax.random.split(jax.random.fold_in(key_list[1], 1), TOKENS // TOK_DEV)
    expert_ids_turns = jax.random.permutation(jax.random.fold_in(key_list[1], 3), TOKENS // TOK_DEV)
    expert_ids = jax.vmap(lambda own, number: assign_block(jax.random.fold_in(key_list[1], 2), own, number, TOK_DEV, EXPERTS, TOP, CAP, 2))(expert_ids_keys, expert_ids_turns).reshape((TOKENS, TOP))
    gate_weight = bell_draw(key_list[2], (D, EXPERTS), D ** -0.5, 0.09375, ((0, 4),))
    reduce_weight = bell_draw(key_list[3], (EXPERTS, D, RANK), D ** -0.5, 0.09375, ((0, 4), (1, 8)))
    middle_weight = bell_draw(key_list[4], (EXPERTS, RANK, RANK), RANK ** -0.5, 0.375, ((0, 4), (1, 2)))
    expand_weight = bell_draw(key_list[5], (EXPERTS, D, RANK), RANK ** -0.5, 0.375, ((0, 4), (1, 8)))
    bias = bell_draw(key_list[6], (D,), 0.5, 3.0, ((0, 4),), jnp.float32)
    return {"inputs": inputs, "expert_ids": expert_ids, "gate_weight": gate_weight, "reduce_weight": reduce_weight, "middle_weight": middle_weight, "expand_weight": expand_weight, "bias": bias}


def pick_rows(expert_rows, slot_pick):
    return expert_rows[slot_pick]


def reference(inputs, expert_ids, gate_weight, reduce_weight, middle_weight, expand_weight, bias):
    weight_tables = (gate_weight, reduce_weight, middle_weight, expand_weight, bias)
    return cross_layer(inputs, expert_ids, weight_tables)


def cross_layer(inputs, expert_ids, tables):
    gate_w, reduce_w, middle_w, expand_w, bias_w = tables

    def group_step(group):
        tokens_in, chosen_ids = group
        numbers = jnp.arange(EXPERTS, dtype=jnp.int32)
        logits = jnp.dot(tokens_in, gate_w, preferred_element_type=jnp.float32)
        chosen = jnp.sum((chosen_ids[:, :, None] == numbers[None, None, :]).astype(jnp.int32), axis=1)
        position = jnp.cumsum(chosen, axis=0).astype(jnp.int32) - chosen
        target = jnp.where(chosen > 0, position, CAP).astype(jnp.int32).T
        expert_grid = jnp.broadcast_to(numbers[:, None], (EXPERTS, TOK_DEV))
        token_grid = jnp.broadcast_to(jnp.arange(TOK_DEV, dtype=jnp.int32)[None, :], (EXPERTS, TOK_DEV))
        slot_owner = jnp.full((EXPERTS, CAP), TOK_DEV, jnp.int32).at[expert_grid, target].set(token_grid, mode="drop")
        padded = jnp.concatenate([tokens_in, jnp.zeros((1, D), tokens_in.dtype)], axis=0)
        dispatched = padded[slot_owner]
        projected = jnp.einsum("esd,edr->esr", dispatched.astype(jnp.float32), reduce_w.astype(jnp.float32))
        squashed = jnp.tanh(projected).astype(jnp.bfloat16)
        inner_mix = jnp.einsum("esj,eij->esi", squashed.astype(jnp.float32), middle_w.astype(jnp.float32))
        hidden = jnp.tanh(inner_mix).astype(jnp.bfloat16)
        expanded = jnp.einsum("esr,edr->esd", hidden.astype(jnp.float32), expand_w.astype(jnp.float32))
        slot_read = jnp.minimum(position, CAP - 1).astype(jnp.int32).T
        picked = jax.vmap(pick_rows)(expanded, slot_read)
        gate_values = jax.nn.sigmoid(logits) * chosen.astype(jnp.float32)
        weighted = gate_values.T[:, :, None] * (picked + bias_w.astype(jnp.float32)[None, None, :])
        per_group = jnp.sum(weighted.reshape(N_EXPERT, EXPERTS // N_EXPERT, TOK_DEV, D), axis=1)
        partial_terms = (tokens_in.astype(jnp.float32)[None] * per_group).astype(jnp.bfloat16)
        partial_terms = lax.optimization_barrier(partial_terms).astype(jnp.float32)
        return (tokens_in.astype(jnp.float32) + jnp.sum(partial_terms, axis=0)).astype(jnp.bfloat16)

    grouped = (inputs.reshape(N_BATCH, TOK_DEV, D), expert_ids.reshape(N_BATCH, TOK_DEV, TOP))
    crossed = lax.map(group_step, grouped)
    return crossed.reshape(TOKENS, D)
```

```python
import functools

import jax
import jax.numpy as jnp
from jax import lax
from jax.experimental import pallas as pl
from jax.experimental.pallas import tpu as pltpu
from jax.sharding import PartitionSpec as P


F32 = jnp.float32
BF16 = jnp.bfloat16
LAST = (((1,), (1,)), ((), ()))


def peer_to(i, m, n):
    return i ^ m if n & (n - 1) == 0 else (i + m) % n


def peer_from(i, m, n):
    return i ^ m if n & (n - 1) == 0 else (i - m + n) % n


def send(x, axis, m, n):
    return lax.ppermute(x, axis, [(i, peer_to(i, m, n)) for i in range(n)])


def any_spec():
    return pl.BlockSpec(memory_space=pl.ANY)


def vmem_spec():
    return pl.BlockSpec(memory_space=pltpu.VMEM)


def smem_spec():
    return pl.BlockSpec(memory_space=pltpu.SMEM)


def project(rows_idx, piece_idx, x, pieces, gate_t, with_logits):
    count = rows_idx.shape[0]
    n_loc, width, rank = pieces[0].shape
    feats = x.shape[1]
    n_piece = len(pieces)
    block = with_logits[1]

    def body(rows_ref, piece_ref, x_ref, *refs):
        w_refs = refs[:n_piece]
        g_ref = refs[n_piece]
        outs = refs[n_piece + 1 : n_piece + 1 + count]
        step = pl.program_id(0)
        xs = [
            x_ref[:, pl.ds(pl.multiple_of(piece_ref[p] * width, width), width)]
            for p in range(n_piece)
        ]
        cols = []
        for e in range(n_loc):
            acc = jnp.dot(xs[0], w_refs[0][e], preferred_element_type=F32)
            for p in range(1, n_piece):
                acc = acc + jnp.dot(xs[p], w_refs[p][e], preferred_element_type=F32)
            cols.append(acc.astype(BF16))
        for k in range(count):

            @pl.when(step == k)
            def _(k=k):
                for e in range(n_loc):
                    outs[k][:, e * rank : (e + 1) * rank] = cols[e]

        if with_logits[0]:

            @pl.when(step == count - 1)
            def _():
                refs[-1][...] = lax.dot_general(
                    g_ref[...], x_ref[...], LAST, preferred_element_type=F32
                )

    out_shape = [jax.ShapeDtypeStruct((block, n_loc * rank), BF16) for _ in range(count)]
    out_specs = [
        pl.BlockSpec((block, n_loc * rank), lambda i, r, p: (0, 0)) for _ in range(count)
    ]
    if with_logits[0]:
        out_shape.append(jax.ShapeDtypeStruct((gate_t.shape[0], block), F32))
        out_specs.append(pl.BlockSpec((gate_t.shape[0], block), lambda i, r, p: (0, 0)))
    return pl.pallas_call(
        body,
        grid_spec=pltpu.PrefetchScalarGridSpec(
            num_scalar_prefetch=2,
            grid=(count,),
            in_specs=[pl.BlockSpec((block, feats), lambda i, r, p: (r[i], 0))]
            + [pl.BlockSpec(w.shape, lambda i, r, p: (0, 0, 0)) for w in pieces]
            + [pl.BlockSpec(gate_t.shape, lambda i, r, p: (0, 0))],
            out_specs=out_specs,
        ),
        out_shape=out_shape,
        name="project",
    )(rows_idx, piece_idx, x, *pieces, gate_t)


def rows_of(ids_t):
    top, n = ids_t.shape
    padded = jnp.concatenate([ids_t, jnp.zeros((8 - top, n), ids_t.dtype)], axis=0)
    return padded.T


def pack(chunk_idx, base_idx, ids_t, parts, n_out, top, n_loc):
    rows, wide = parts[0].shape
    rank = wide // n_loc
    per = rows // n_out
    n_part = len(parts)

    def body(chunk_ref, base_ref, ids_ref, *refs):
        p_refs = refs[:n_part]
        outs = refs[n_part : n_part + n_out]
        scratch = refs[-1]
        scratch[...] = rows_of(ids_ref[...])
        for m in range(n_out):
            sl = pl.ds(pl.multiple_of(chunk_ref[m] * per, per), per)
            ids = scratch[sl, :]
            for j in range(top):
                mine = ids[:, j : j + 1]
                acc = jnp.zeros((per, rank), BF16)
                for q in range(n_part):
                    for e in range(n_loc):
                        acc = jnp.where(
                            mine == base_ref[q] + e,
                            p_refs[q][sl, e * rank : (e + 1) * rank],
                            acc,
                        )
                outs[m][:, j * rank : (j + 1) * rank] = acc

    return pl.pallas_call(
        body,
        in_specs=[smem_spec(), smem_spec()] + [vmem_spec()] * (1 + n_part),
        out_specs=[vmem_spec()] * n_out,
        out_shape=[jax.ShapeDtypeStruct((per, top * rank), BF16) for _ in range(n_out)],
        scratch_shapes=[pltpu.VMEM((rows, 8), jnp.int32)],
        name="pack",
    )(chunk_idx, base_idx, ids_t, *parts)


def mix(own_chunk, base_idx, piece_idx, ids_t, parts, mids, top):
    per, wide = parts[0].shape
    rank = wide // top
    n_part = len(parts)
    n_piece = len(mids[0])
    n_loc, half, _ = mids[0][0].shape
    n_src = len(mids)
    flat = [w for group in mids for w in group]

    def body(chunk_ref, base_ref, piece_ref, ids_ref, *refs):
        p_refs = refs[:n_part]
        m_refs = refs[n_part : n_part + len(flat)]
        out_ref = refs[n_part + len(flat)]
        ids_scratch, squash = refs[-2], refs[-1]
        ids_scratch[...] = rows_of(ids_ref[...])
        ids = ids_scratch[pl.ds(pl.multiple_of(chunk_ref[0] * per, per), per), :]
        masks = []
        for j in range(top):
            cols = slice(j * rank, (j + 1) * rank)
            acc = p_refs[0][:, cols].astype(F32)
            for p in range(1, n_part):
                acc = acc + p_refs[p][:, cols].astype(F32)
            squash[j * per : (j + 1) * per, :] = jnp.tanh(acc).astype(BF16)
            masks.append(ids[:, j : j + 1])
        mine = jnp.concatenate(masks, axis=0)
        sq = squash[...]
        for h in range(n_piece):
            acc = jnp.zeros((top * per, half), F32)
            for q in range(n_src):
                for e in range(n_loc):
                    got = lax.dot_general(
                        sq, m_refs[q * n_piece + h][e], LAST, preferred_element_type=F32
                    )
                    acc = jnp.where(mine == base_ref[q] + e, got, acc)
            hid = jnp.tanh(acc).astype(BF16)
            for j in range(top):
                start = pl.multiple_of(j * rank + piece_ref[h] * half, half)
                out_ref[:, pl.ds(start, half)] = hid[j * per : (j + 1) * per, :]

    return pl.pallas_call(
        body,
        in_specs=[smem_spec()] * 3 + [vmem_spec()] * (1 + n_part + len(flat)),
        out_specs=vmem_spec(),
        out_shape=jax.ShapeDtypeStruct((per, wide), BF16),
        scratch_shapes=[
            pltpu.VMEM((ids_t.shape[1], 8), jnp.int32),
            pltpu.VMEM((top * per, rank), BF16),
        ],
        name="mix",
    )(own_chunk, base_idx, piece_idx, ids_t, *parts, *flat)


def expand(own_block, chunk_idx, base_idx, piece_idx, x, ids_t, bias, logits, hids, wides, top):
    per, wide = hids[0].shape
    rank = wide // top
    n_hid = len(hids)
    n_log = len(logits)
    rows = per * n_hid
    feats = x.shape[1]
    n_src = len(wides)
    n_piece = len(wides[0])
    n_loc, half, _ = wides[0][0].shape
    flat = [w for group in wides for w in group]
    n_flat = len(flat)

    def body(block_ref, chunk_ref, base_ref, piece_ref, x_ref, ids_ref, bias_ref, *refs):
        l_refs = refs[:n_log]
        h_refs = refs[n_log : n_log + n_hid]
        w_refs = refs[n_log + n_hid : n_log + n_hid + n_flat]
        out_ref = refs[n_log + n_hid + n_flat]
        w_bufs = refs[n_log + n_hid + n_flat + 1 : n_log + n_hid + 2 * n_flat + 1]
        hid, left, gate_s, ids_s, sems = refs[n_log + n_hid + 2 * n_flat + 1 :]
        copies = [
            pltpu.make_async_copy(w_refs[k], w_bufs[k], sems.at[k]) for k in range(n_flat)
        ]
        for c in copies:
            c.start()
        logit = l_refs[0][...]
        for k in range(1, n_log):
            logit = logit + l_refs[k][...]
        gate_s[...] = jax.nn.sigmoid(logit).T
        ids_s[...] = rows_of(ids_ref[...])
        for k in range(n_hid):
            hid[pl.ds(pl.multiple_of(chunk_ref[k] * per, per), per), :] = h_refs[k][...]
        ids = ids_s[...]
        gates = gate_s[...]
        total = jnp.zeros((rows, 1), F32)
        lane = lax.broadcasted_iota(jnp.int32, gates.shape, 1)
        for q in range(n_src):
            for e in range(n_loc):
                number = base_ref[q] + e
                gate = jnp.sum(jnp.where(lane == number, gates, 0.0), axis=1, keepdims=True)
                acc = jnp.zeros((rows, rank), F32)
                here = jnp.zeros((rows, 1), F32)
                for j in range(top):
                    hit = ids[:, j : j + 1] == number
                    acc = jnp.where(hit, hid[:, j * rank : (j + 1) * rank].astype(F32), acc)
                    here = jnp.where(hit, gate, here)
                left[q * n_loc + e] = (acc * here).astype(BF16)
                total = total + here
        for h in range(n_piece):
            acc = jnp.zeros((rows, half), F32)
            for q in range(n_src):
                copies[q * n_piece + h].wait()
                for e in range(n_loc):
                    acc = acc + lax.dot_general(
                        left[q * n_loc + e],
                        w_bufs[q * n_piece + h][e],
                        LAST,
                        preferred_element_type=F32,
                    )
            cols = pl.ds(pl.multiple_of(piece_ref[h] * half, half), half)
            xs = x_ref[:, cols].astype(F32)
            mixed = acc + total * bias_ref[:, cols]
            out_ref[:, cols] = (xs + xs * mixed).astype(BF16)

    return pl.pallas_call(
        body,
        grid_spec=pltpu.PrefetchScalarGridSpec(
            num_scalar_prefetch=4,
            grid=(1,),
            in_specs=[
                pl.BlockSpec((rows, feats), lambda i, a, b, c, d: (a[0], 0)),
                vmem_spec(),
                vmem_spec(),
            ]
            + [vmem_spec()] * (n_log + n_hid)
            + [any_spec()] * n_flat,
            out_specs=pl.BlockSpec((rows, feats), lambda i, a, b, c, d: (0, 0)),
            scratch_shapes=[pltpu.VMEM(w.shape, BF16) for w in flat]
            + [
                pltpu.VMEM((rows, wide), BF16),
                pltpu.VMEM((n_src * n_loc, rows, rank), BF16),
                pltpu.VMEM((rows, logits[0].shape[0]), F32),
                pltpu.VMEM((rows, 8), jnp.int32),
                pltpu.SemaphoreType.DMA((n_flat,)),
            ],
        ),
        out_shape=jax.ShapeDtypeStruct((rows, feats), BF16),
        name="expand",
    )(own_block, chunk_idx, base_idx, piece_idx, x, ids_t, bias, *logits, *hids, *flat)


def on_device(
    nb, ne, nz, inputs, expert_ids, gate_weight, reduce_weight, middle_weight, expand_weight, bias
):
    tok, feats = inputs.shape
    top = expert_ids.shape[1]
    n_loc = reduce_weight.shape[0]
    block = tok // ne
    b = lax.axis_index("batch")
    x_at = lax.axis_index("expert")
    z_at = lax.axis_index("dim")
    as_vec = lambda vals: jnp.stack([jnp.asarray(v, jnp.int32) for v in vals])
    pair = nb == 2
    piece_idx = as_vec([b, 1 - b]) if pair else as_vec([0])

    def both(w):
        return [w, lax.ppermute(w, "batch", [(0, 1), (1, 0)])]

    def whole(w):
        return lax.all_gather(w, "batch", axis=1, tiled=True)

    reduce_pieces = both(reduce_weight) if pair else [whole(reduce_weight)]
    gate_t = gate_weight.T
    ids_t = lax.dynamic_slice_in_dim(expert_ids.T, x_at * block, block, 1)
    far = as_vec([peer_to(x_at, m, ne) for m in range(ne - 1, 0, -1)])
    sent = project(far, piece_idx, inputs, reduce_pieces, gate_t, (False, block))
    got = [send(s, "expert", m, ne) for s, m in zip(sent, range(ne - 1, 0, -1))]
    own, logit = project(as_vec([x_at]), piece_idx, inputs, reduce_pieces, gate_t, (True, block))
    logits = [logit] + [send(logit, "dim", m, nz) for m in range(1, nz)]

    def spread(w):
        if not pair:
            w = whole(w)
        held = [w] + [send(w, "expert", m, ne) for m in range(1, ne)]
        return [both(h) if pair else [h] for h in held]

    mids = spread(middle_weight)
    wides = spread(expand_weight)
    parts = [own] + got[::-1]
    base = as_vec([peer_from(x_at, m, ne) * n_loc for m in range(ne)])
    chunk_to = as_vec([peer_to(z_at, m, nz) for m in range(nz)])
    chunk_from = as_vec([peer_from(z_at, m, nz) for m in range(nz)])
    packed = pack(chunk_to, base, ids_t, parts, nz, top, n_loc)
    sums = [packed[0]] + [send(packed[m], "dim", m, nz) for m in range(nz - 1, 0, -1)]
    hid = mix(as_vec([z_at]), base, piece_idx, ids_t, sums, mids, top)
    hids = [hid] + [send(hid, "dim", m, nz) for m in range(1, nz)]
    return expand(
        as_vec([x_at]), chunk_from, base, piece_idx, inputs, ids_t, bias[None, :],
        logits, hids, wides, top,
    )


def solution(mesh):
    sizes = dict(mesh.shape)
    in_specs = (
        P("batch", "dim"),
        P("batch", None),
        P("dim", None),
        P("expert", ("dim", "batch"), None),
        P("expert", "batch", None),
        P("expert", ("dim", "batch"), None),
        P("dim"),
    )
    out_specs = P(("batch", "expert"), "dim")
    body = functools.partial(on_device, sizes["batch"], sizes["expert"], sizes["dim"])
    return jax.shard_map(body, mesh=mesh, in_specs=in_specs, out_specs=out_specs, check_vma=False)
```

```python
import jax
import jax.numpy as jnp
from jax import lax
from jax.experimental import pallas as pl
from jax.experimental.pallas import tpu as pltpu
from jax.sharding import PartitionSpec as P


F32 = jnp.float32
BF16 = jnp.bfloat16
LAST = (((1,), (1,)), ((), ()))
MIB = 1 << 20
SPLIT = 2


def peer_to(i, m, n):
    return i ^ m if n & (n - 1) == 0 else (i + m) % n


def peer_from(i, m, n):
    return i ^ m if n & (n - 1) == 0 else (i - m + n) % n


def send(x, axis, m, n):
    return lax.ppermute(x, axis, [(i, peer_to(i, m, n)) for i in range(n)])


def vmem():
    return pl.BlockSpec(memory_space=pltpu.VMEM)


def call(body, args, outs, scratch=(), limit=12, flops=None, held=(), alias=None):
    space = lambda k: pl.BlockSpec(memory_space=pl.ANY) if k in held else vmem()
    cost = None if flops is None else pl.CostEstimate(flops, 0, flops // 500)
    return pl.pallas_call(
        body,
        in_specs=[pl.BlockSpec(memory_space=pltpu.SMEM)] + [space(k) for k in range(1, len(args))],
        out_specs=[space("out") for _ in outs],
        out_shape=[jax.ShapeDtypeStruct(s, t) for s, t in outs],
        scratch_shapes=list(scratch),
        input_output_aliases={} if alias is None else {alias: 0},
        cost_estimate=cost,
        compiler_params=pltpu.CompilerParams(vmem_limit_bytes=limit * MIB),
    )(*args)


def rows_at(start, size):
    return pl.ds(pl.multiple_of(start, size), size)


def as_rows(cols_t):
    top, n = cols_t.shape
    pad = jnp.zeros((8 - top, n), cols_t.dtype)
    return jnp.concatenate([cols_t, pad], axis=0).T


def project(place, x, pieces, row_starts, n_row, pair, gate_t=None):
    n_loc, width, rank = pieces[0].shape
    n_piece = len(pieces)
    count = row_starts[1]

    def body(place_ref, x_ref, *refs):
        w_refs, outs = refs[:n_piece], refs[n_piece:]
        starts = row_starts[0](place_ref)
        first = [place_ref[0], 1 - place_ref[0]] if pair else [0]
        xs = []
        for p in range(n_piece):
            cols = rows_at(first[p] * width, width)
            xs.append(jnp.concatenate([x_ref[rows_at(s, n_row), cols] for s in starts], axis=0))
        if gate_t is not None:
            logit = None
            for p in range(n_piece):
                part = lax.dot_general(
                    outs[0][:, rows_at(first[p] * width, width)], xs[p], LAST,
                    preferred_element_type=F32,
                )
                logit = part if logit is None else logit + part
            outs[-1][...] = logit
            outs = outs[1:]
        for e in range(n_loc):
            acc = jnp.dot(xs[0], w_refs[0][e], preferred_element_type=F32)
            for p in range(1, n_piece):
                acc = acc + jnp.dot(xs[p], w_refs[p][e], preferred_element_type=F32)
            acc = acc.astype(BF16)
            for k in range(count):
                outs[k][:, e * rank : (e + 1) * rank] = acc[k * n_row : (k + 1) * n_row]

    args = [place, x, *pieces]
    outs = [((n_row, n_loc * rank), BF16)] * count
    if gate_t is not None:
        args.append(gate_t)
        outs = outs + [((gate_t.shape[0], n_row * count), F32)]
    return call(body, args, outs)


def widen(place, wide):
    n_loc, half, rank = wide.shape

    def body(place_ref, w_ref, out_ref, buf, sem):
        copy = pltpu.make_async_copy(w_ref, buf, sem)
        copy.start()
        copy.wait()
        for e in range(n_loc):
            out_ref[e] = buf[e].T

    return call(
        body, [place, wide], [((n_loc, rank, half), BF16)],
        [pltpu.VMEM(wide.shape, BF16), pltpu.SemaphoreType.DMA], flops=4_000_000_000, held=(1,),
    )[0]


def turn(place, mids):
    n_loc, half, rank = mids[0].shape

    def body(place_ref, *refs):
        for q in range(len(mids)):
            for e in range(n_loc):
                refs[-1][q * n_loc + e] = refs[q][e].T

    return call(body, [place, *mids], [((len(mids) * n_loc, rank, half), BF16)])[0]


def wide_ids(ids_ref, start, n, width):
    ids = as_rows(ids_ref[:, rows_at(start, n)].astype(F32))
    top = ids_ref.shape[0]
    return [jnp.broadcast_to(ids[:, j : j + 1], (n, width)).astype(BF16) for j in range(top)]


def pack(place, ids_t, parts, at, n_expert, n_dim, n_loc, logit=None):
    rows, wide = parts[0].shape
    rank = wide // n_loc
    per = rows // n_dim
    top = ids_t.shape[0]
    n_part = len(parts)
    more = 0 if logit is None else logit.shape[0]

    def body(place_ref, ids_ref, *refs):
        p_refs, scratch = refs[:n_part], refs[-1]
        outs = refs[n_part:-1] if logit is None else refs[n_part + 1 : -1]
        x_at, z_at = place_ref[1], place_ref[2]
        ids = wide_ids(ids_ref, x_at * (rows * SPLIT) + at * rows, rows, rank)
        for j in range(top):
            acc = jnp.zeros((rows, rank), BF16)
            for q in range(n_part):
                base = peer_from(x_at, q, n_expert) * n_loc
                for e in range(n_loc):
                    number = (base + e).astype(F32).astype(BF16)
                    acc = jnp.where(
                        ids[j] == number, p_refs[q][:, e * rank : (e + 1) * rank], acc
                    )
            scratch[:, j * rank : (j + 1) * rank] = acc
        for m in range(n_dim):
            outs[m][:per, :] = scratch[rows_at(peer_to(z_at, m, n_dim) * per, per), :]
        if logit is not None:
            full = refs[n_part][...]
            n = full.shape[1]
            high = full.astype(BF16)
            low = (full - high.astype(F32)).astype(BF16)
            for m in range(n_dim):
                outs[m][per:, :n] = high
                outs[m][per:, n : 2 * n] = low
                outs[m][per:, 2 * n :] = jnp.zeros((more, top * rank - 2 * n), BF16)

    return call(
        body,
        [place, ids_t, *parts] + ([] if logit is None else [logit]),
        [((per + more, top * rank), BF16)] * n_dim,
        [pltpu.VMEM((rows, top * rank), BF16)],
    )


def mix(place, ids_t, gates_t, parts, mids, at, block, n_expert, n_dim, pair):
    wide = parts[0].shape[1]
    top, _ = ids_t.shape
    rank = wide // top
    per = block // SPLIT // n_dim
    n_part = len(parts)
    n_piece = len(mids)
    n_all, _, half = mids[0].shape
    n_loc = n_all // n_expert
    make = gates_t is None

    def body(place_ref, ids_ref, *refs):
        if make:
            p_refs, refs = refs[:n_part], refs[n_part:]
        else:
            g_ref, p_refs, refs = refs[0], refs[1 : n_part + 1], refs[n_part + 1 :]
        m_refs, refs = refs[:n_piece], refs[n_piece:]
        if make:
            out_ref, g_out, squash, ids_s, gate_s = refs
            logit = jnp.zeros((n_all, block), F32)
            for p in range(n_part):
                logit = logit + p_refs[p][per:, :block].astype(F32)
                logit = logit + p_refs[p][per:, block : 2 * block].astype(F32)
            gates_t = jax.nn.sigmoid(logit)
            g_out[...] = gates_t
        else:
            out_ref, squash, ids_s, gate_s = refs
            gates_t = g_ref[...]
        x_at, z_at = place_ref[1], place_ref[2]
        first = [place_ref[0], 1 - place_ref[0]] if pair else [0]
        ids_s[...] = as_rows(ids_ref[:, rows_at(x_at * block, block)])
        gate_s[...] = gates_t.T
        mine = rows_at(at * per * n_dim + z_at * per, per)
        ids, gates = ids_s[mine, :], gate_s[mine, :]
        lane = lax.broadcasted_iota(jnp.int32, gates.shape, 1)
        chosen, gate = [], []
        for j in range(top):
            cols = slice(j * rank, (j + 1) * rank)
            acc = p_refs[0][:per, cols].astype(F32)
            for p in range(1, n_part):
                acc = acc + p_refs[p][:per, cols].astype(F32)
            squash[j * per : (j + 1) * per, :] = jnp.tanh(acc).astype(BF16)
            own = ids[:, j : j + 1]
            chosen.append(own)
            gate.append(jnp.sum(jnp.where(lane == own, gates, 0.0), axis=1, keepdims=True))
        chosen = jnp.broadcast_to(jnp.concatenate(chosen, axis=0), (top * per, half))
        sq = squash[...]
        for h in range(n_piece):
            acc = jnp.zeros((top * per, half), F32)
            for q in range(n_expert):
                base = peer_from(x_at, q, n_expert) * n_loc
                for e in range(n_loc):
                    got = jnp.dot(sq, m_refs[h][q * n_loc + e], preferred_element_type=F32)
                    acc = jnp.where(chosen == base + e, got, acc)
            hid = jnp.tanh(acc)
            for j in range(top):
                start = pl.multiple_of(j * rank + first[h] * half, half)
                gated = hid[j * per : (j + 1) * per, :] * gate[j]
                out_ref[:, pl.ds(start, half)] = gated.astype(BF16)

    return call(
        body,
        [place, ids_t] + ([] if make else [gates_t]) + [*parts, *mids],
        [((per, wide), BF16)] + ([((n_all, block), F32)] if make else []),
        [
            pltpu.VMEM((top * per, rank), BF16),
            pltpu.VMEM((block, 8), jnp.int32),
            pltpu.VMEM((block, n_all), F32),
        ],
    )


def expand(place, x, ids_t, bias, gates_t, hids, wides, at, so_far, n_expert, n_dim, n_loc, pair):
    per, wide = hids[0].shape
    top, _ = ids_t.shape
    rank = wide // top
    rows = per * n_dim
    block = rows * SPLIT
    feats = x.shape[1]
    n_src = len(wides)
    n_piece = len(wides[0])
    half = wides[0][0].shape[2]
    flat_w = [w for src in wides for w in src]
    n_h, n_w = len(hids), len(flat_w)
    n_first = 0 if so_far is None else 1

    def body(place_ref, *refs):
        refs = refs[n_first:]
        x_ref, ids_ref, bias_ref, g_ref, *refs = refs
        h_refs, w_refs = refs[:n_h], refs[n_h : n_h + n_w]
        out_ref, hid, left, buf, sems = refs[n_h + n_w :]
        x_at, z_at = place_ref[1], place_ref[2]
        first = [place_ref[0], 1 - place_ref[0]] if pair else [0]
        mine = rows_at(x_at * block + at * rows, rows)
        for m in range(n_dim):
            hid[rows_at(peer_from(z_at, m, n_dim) * per, per), :] = h_refs[m][...]
        ids = wide_ids(ids_ref, x_at * block + at * rows, rows, rank)
        for q in range(n_src):
            base = peer_from(x_at, q, n_expert) * n_loc
            for e in range(n_loc):
                number = (base + e).astype(F32).astype(BF16)
                acc = jnp.zeros((rows, rank), BF16)
                for j in range(top):
                    acc = jnp.where(ids[j] == number, hid[:, j * rank : (j + 1) * rank], acc)
                left[q * n_loc + e] = acc
        own = ids_ref[:, mine]
        gates = g_ref[:, at * rows : (at + 1) * rows]
        number = lax.broadcasted_iota(jnp.int32, gates.shape, 0)
        hit = own[0:1, :] == number
        for j in range(1, top):
            hit = hit | (own[j : j + 1, :] == number)
        total = jnp.sum(jnp.where(hit, gates, 0.0), axis=0, keepdims=True)
        total = jnp.broadcast_to(total, gates.shape).T[:, 0:1]
        copies = []
        for h in range(n_piece):
            acc = jnp.zeros((rows, half), F32)
            for q in range(n_src):
                for e in range(n_loc):
                    w = w_refs[q * n_piece + h][e]
                    acc = acc + jnp.dot(left[q * n_loc + e], w, preferred_element_type=F32)
            cols = rows_at(first[h] * half, half)
            xs = x_ref[mine, cols].astype(F32)
            buf[h] = (xs + xs * (acc + total * bias_ref[:, cols])).astype(BF16)
            there = out_ref.at[at * rows : (at + 1) * rows, cols]
            copies.append(pltpu.make_async_copy(buf.at[h], there, sems.at[h]))
            copies[-1].start()
        for c in copies:
            c.wait()

    args = [place] + ([] if so_far is None else [so_far])
    return call(
        body,
        args + [x, ids_t, bias, gates_t, *hids, *flat_w],
        [((block, feats), BF16)],
        [
            pltpu.VMEM((rows, wide), BF16),
            pltpu.VMEM((n_src * n_loc, rows, rank), BF16),
            pltpu.VMEM((n_piece, rows, half), BF16),
            pltpu.SemaphoreType.DMA((n_piece,)),
        ],
        held=("out",) if so_far is None else ("out", 1),
        alias=None if so_far is None else 1,
    )[0]


def on_device(
    nb, ne, nz, inputs, expert_ids, gate_weight, reduce_weight, middle_weight, expand_weight, bias
):
    tok, _ = inputs.shape
    n_loc = reduce_weight.shape[0]
    block = tok // ne
    n_row = block // SPLIT
    pair = nb == 2
    place = jnp.stack([lax.axis_index(a).astype(jnp.int32) for a in ("batch", "expert", "dim")])
    ids_t = expert_ids.T

    def swap(w):
        return lax.ppermute(w, "batch", [(0, 1), (1, 0)])

    def whole(w):
        return lax.all_gather(w, "batch", axis=1, tiled=True)

    if pair:
        pieces = [reduce_weight, swap(reduce_weight)]
    else:
        pieces = [whole(reduce_weight)]
        middle_weight, expand_weight = whole(middle_weight), whole(expand_weight)
    far = list(range(1, ne))
    wide = widen(place, expand_weight)
    mids = [middle_weight] + [send(middle_weight, "expert", m, ne) for m in far]

    parts = []
    for h in range(SPLIT):
        starts = lambda r, h=h: [peer_to(r[1], m, ne) * block + h * n_row for m in far]
        sent = project(place, inputs, pieces, (starts, len(far)), n_row, pair)
        parts.append([send(s, "expert", m, ne) for s, m in zip(sent, far)])
    starts = lambda r: [r[1] * block + h * n_row for h in range(SPLIT)]
    *own, logit = project(place, inputs, pieces, (starts, SPLIT), n_row, pair, gate_weight.T)
    wides = [wide] + [send(wide, "expert", m, ne) for m in far]
    mids = [turn(place, mids)]
    if pair:
        mids.append(swap(mids[0]))

    sums = []
    for h in range(SPLIT):
        packed = pack(
            place, ids_t, [own[h]] + parts[h], h, ne, nz, n_loc, logit if h == 0 else None
        )
        sums.append([packed[0]] + [send(packed[m], "dim", m, nz) for m in range(1, nz)])
    hids, gates_t = [], None
    for h in range(SPLIT):
        hid, *made = mix(place, ids_t, gates_t, sums[h], mids, h, block, ne, nz, pair)
        gates_t = made[0] if made else gates_t
        hids.append([hid] + [send(hid, "dim", m, nz) for m in range(1, nz)])
    wides = [[w] + ([swap(w)] if pair else []) for w in wides]
    out = None
    for h in range(SPLIT):
        out = expand(
            place, inputs, ids_t, bias[None, :], gates_t, hids[h], wides, h, out, ne, nz, n_loc,
            pair,
        )
    return out


def solution(mesh):
    sizes = dict(mesh.shape)
    in_specs = (
        P("batch", "dim"),
        P("batch", None),
        P("dim", None),
        P("expert", ("dim", "batch"), None),
        P("expert", "batch", None),
        P("expert", ("dim", "batch"), None),
        P("dim"),
    )
    out_specs = P(("batch", "expert"), "dim")
    nb, ne, nz = sizes["batch"], sizes["expert"], sizes["dim"]

    def body(*args):
        return on_device(nb, ne, nz, *args)

    return jax.shard_map(body, mesh=mesh, in_specs=in_specs, out_specs=out_specs, check_vma=False)
```

```python
import jax
import jax.numpy as jnp
from jax import lax
from jax.experimental import pallas as pl
from jax.experimental.pallas import tpu as pltpu
from jax.sharding import PartitionSpec as P


F32 = jnp.float32
BF16 = jnp.bfloat16
LAST = (((1,), (1,)), ((), ()))
MIB = 1 << 20
SPLIT = 2


def peer_to(i, m, n):
    return i ^ m if n & (n - 1) == 0 else (i + m) % n


def peer_from(i, m, n):
    return i ^ m if n & (n - 1) == 0 else (i - m + n) % n


def send(x, axis, m, n):
    return lax.ppermute(x, axis, [(i, peer_to(i, m, n)) for i in range(n)])


def vmem():
    return pl.BlockSpec(memory_space=pltpu.VMEM)


def call(body, args, outs, scratch=(), limit=12, flops=None, held=(), alias=None):
    space = lambda k: pl.BlockSpec(memory_space=pl.ANY) if k in held else vmem()
    cost = None if flops is None else pl.CostEstimate(flops, 0, flops // 500)

    def placed(*refs):
        body([lax.axis_index(a) for a in ("batch", "expert", "dim")], *refs)

    return pl.pallas_call(
        placed,
        in_specs=[space(k) for k in range(len(args))],
        out_specs=[space("out") for _ in outs],
        out_shape=[jax.ShapeDtypeStruct(s, t) for s, t in outs],
        scratch_shapes=list(scratch),
        input_output_aliases={} if alias is None else {alias: 0},
        cost_estimate=cost,
        compiler_params=pltpu.CompilerParams(vmem_limit_bytes=limit * MIB),
    )(*args)


def rows_at(start, size):
    return pl.ds(pl.multiple_of(start, size), size)


def as_rows(cols_t):
    top, n = cols_t.shape
    pad = jnp.zeros((8 - top, n), cols_t.dtype)
    return jnp.concatenate([cols_t, pad], axis=0).T


def begin():
    def body(place_ref, out_ref):
        out_ref[...] = jnp.zeros(out_ref.shape, jnp.int32)

    return call(body, [], [((8, 128), jnp.int32)], flops=6_000_000_000)[0]


def project(x, pieces, gate_t, begun, h, n_row, n_expert, pair):
    n_loc, width, rank = pieces[0].shape
    n_piece = len(pieces)
    block = n_row * SPLIT

    def body(place_ref, x_ref, *refs):
        w_refs, g_ref = refs[:n_piece], refs[n_piece]
        logit_ref, *outs = refs[n_piece + 2 :]
        first = [place_ref[0], 1 - place_ref[0]] if pair else [0]
        starts = [
            peer_to(place_ref[1], m, n_expert) * block + h * n_row for m in range(n_expert)
        ]
        xs = []
        for p in range(n_piece):
            cols = rows_at(first[p] * width, width)
            xs.append(jnp.concatenate([x_ref[rows_at(s, n_row), cols] for s in starts], axis=0))
        for e in range(n_loc):
            acc = jnp.dot(xs[0], w_refs[0][e], preferred_element_type=F32)
            for p in range(1, n_piece):
                acc = acc + jnp.dot(xs[p], w_refs[p][e], preferred_element_type=F32)
            acc = acc.astype(BF16)
            for m in range(n_expert):
                outs[m][:, e * rank : (e + 1) * rank] = acc[m * n_row : (m + 1) * n_row]
        logit = None
        for p in range(n_piece):
            gate = g_ref[:, rows_at(first[p] * width, width)]
            part = lax.dot_general(gate, xs[p][:n_row], LAST, preferred_element_type=F32)
            logit = part if logit is None else logit + part
        logit_ref[...] = logit

    return call(
        body,
        [x, *pieces, gate_t, begun],
        [((gate_t.shape[0], n_row), F32)] + [((n_row, n_loc * rank), BF16)] * n_expert,
        flops=3_000_000_000,
    )


def widen(wide):
    n_loc, half, rank = wide.shape

    def body(place_ref, w_ref, out_ref):
        for e in range(n_loc):
            out_ref[e] = w_ref[e].T

    return call(body, [wide], [((n_loc, rank, half), BF16)])[0]


def turn(mids):
    n_loc, half, rank = mids[0].shape

    def body(place_ref, *refs):
        for q in range(len(mids)):
            for e in range(n_loc):
                refs[-1][q * n_loc + e] = refs[q][e].T

    return call(body, [*mids], [((len(mids) * n_loc, rank, half), BF16)])[0]


def wide_ids(ids_ref, start, n, width):
    ids = as_rows(ids_ref[:, rows_at(start, n)].astype(F32))
    top = ids_ref.shape[0]
    return [jnp.broadcast_to(ids[:, j : j + 1], (n, width)).astype(BF16) for j in range(top)]


def pack(ids_t, parts, at, n_expert, n_dim, n_loc, logits=()):
    rows, wide = parts[0].shape
    rank = wide // n_loc
    per = rows // n_dim
    top = ids_t.shape[0]
    n_part = len(parts)
    n_log = len(logits)
    more = logits[0].shape[0] if logits else 0

    def body(place_ref, ids_ref, *refs):
        p_refs, scratch = refs[:n_part], refs[-1]
        l_refs, outs = refs[n_part : n_part + n_log], refs[n_part + n_log : -1]
        x_at, z_at = place_ref[1], place_ref[2]
        ids = wide_ids(ids_ref, x_at * (rows * SPLIT) + at * rows, rows, rank)
        for j in range(top):
            acc = jnp.zeros((rows, rank), BF16)
            for q in range(n_part):
                base = peer_from(x_at, q, n_expert) * n_loc
                for e in range(n_loc):
                    number = (base + e).astype(F32).astype(BF16)
                    acc = jnp.where(
                        ids[j] == number, p_refs[q][:, e * rank : (e + 1) * rank], acc
                    )
            scratch[:, j * rank : (j + 1) * rank] = acc
        for m in range(n_dim):
            outs[m][:per, :] = scratch[rows_at(peer_to(z_at, m, n_dim) * per, per), :]
        if logits:
            full = jnp.concatenate([r[...] for r in l_refs], axis=1)
            n = full.shape[1]
            high = full.astype(BF16)
            low = (full - high.astype(F32)).astype(BF16)
            for m in range(n_dim):
                outs[m][per:, :n] = high
                outs[m][per:, n : 2 * n] = low
                outs[m][per:, 2 * n :] = jnp.zeros((more, top * rank - 2 * n), BF16)

    return call(
        body,
        [ids_t, *parts, *logits],
        [((per + more, top * rank), BF16)] * n_dim,
        [pltpu.VMEM((rows, top * rank), BF16)],
    )


def mix(ids_t, gates_t, parts, mids, at, block, n_expert, n_dim, pair):
    wide = parts[0].shape[1]
    top, _ = ids_t.shape
    rank = wide // top
    per = block // SPLIT // n_dim
    n_part = len(parts)
    n_piece = len(mids)
    n_all, _, half = mids[0].shape
    n_loc = n_all // n_expert
    make = gates_t is None

    def body(place_ref, ids_ref, *refs):
        if make:
            p_refs, refs = refs[:n_part], refs[n_part:]
        else:
            g_ref, p_refs, refs = refs[0], refs[1 : n_part + 1], refs[n_part + 1 :]
        m_refs, refs = refs[:n_piece], refs[n_piece:]
        if make:
            out_ref, g_out, squash, ids_s, gate_s = refs
            logit = jnp.zeros((n_all, block), F32)
            for p in range(n_part):
                logit = logit + p_refs[p][per:, :block].astype(F32)
                logit = logit + p_refs[p][per:, block : 2 * block].astype(F32)
            gates_t = jax.nn.sigmoid(logit)
            g_out[...] = gates_t
        else:
            out_ref, squash, ids_s, gate_s = refs
            gates_t = g_ref[...]
        x_at, z_at = place_ref[1], place_ref[2]
        first = [place_ref[0], 1 - place_ref[0]] if pair else [0]
        ids_s[...] = as_rows(ids_ref[:, rows_at(x_at * block, block)])
        gate_s[...] = gates_t.T
        mine = rows_at(at * per * n_dim + z_at * per, per)
        ids, gates = ids_s[mine, :], gate_s[mine, :]
        lane = lax.broadcasted_iota(jnp.int32, gates.shape, 1)
        chosen, gate = [], []
        for j in range(top):
            cols = slice(j * rank, (j + 1) * rank)
            acc = p_refs[0][:per, cols].astype(F32)
            for p in range(1, n_part):
                acc = acc + p_refs[p][:per, cols].astype(F32)
            squash[j * per : (j + 1) * per, :] = jnp.tanh(acc).astype(BF16)
            own = ids[:, j : j + 1]
            chosen.append(own)
            gate.append(jnp.sum(jnp.where(lane == own, gates, 0.0), axis=1, keepdims=True))
        chosen = jnp.broadcast_to(jnp.concatenate(chosen, axis=0), (top * per, half))
        sq = squash[...]
        for h in range(n_piece):
            acc = jnp.zeros((top * per, half), F32)
            for q in range(n_expert):
                base = peer_from(x_at, q, n_expert) * n_loc
                for e in range(n_loc):
                    got = jnp.dot(sq, m_refs[h][q * n_loc + e], preferred_element_type=F32)
                    acc = jnp.where(chosen == base + e, got, acc)
            hid = jnp.tanh(acc)
            for j in range(top):
                start = pl.multiple_of(j * rank + first[h] * half, half)
                gated = hid[j * per : (j + 1) * per, :] * gate[j]
                out_ref[:, pl.ds(start, half)] = gated.astype(BF16)

    return call(
        body,
        [ids_t] + ([] if make else [gates_t]) + [*parts, *mids],
        [((per, wide), BF16)] + ([((n_all, block), F32)] if make else []),
        [
            pltpu.VMEM((top * per, rank), BF16),
            pltpu.VMEM((block, 8), jnp.int32),
            pltpu.VMEM((block, n_all), F32),
        ],
    )


def expand(x, ids_t, bias, gates_t, hids, wides, at, n_expert, n_dim, n_loc, pair):
    per, wide = hids[0].shape
    top, _ = ids_t.shape
    rank = wide // top
    rows = per * n_dim
    block = rows * SPLIT
    feats = x.shape[1]
    n_src = len(wides)
    n_piece = len(wides[0])
    half = wides[0][0].shape[2]
    flat_w = [w for src in wides for w in src]
    n_h, n_w = len(hids), len(flat_w)
    later = n_expert - n_src

    def body(place_ref, ids_ref, bias_ref, g_ref, *refs):
        h_refs, w_refs = refs[:n_h], refs[n_h : n_h + n_w]
        out_ref, later_ref, hid, left = refs[n_h + n_w :]
        x_at, z_at = place_ref[1], place_ref[2]
        first = [place_ref[0], 1 - place_ref[0]] if pair else [0]
        for m in range(n_dim):
            hid[rows_at(peer_from(z_at, m, n_dim) * per, per), :] = h_refs[m][...]
        ids = wide_ids(ids_ref, x_at * block + at * rows, rows, rank)
        for q in range(n_expert):
            base = peer_from(x_at, q, n_expert) * n_loc
            for e in range(n_loc):
                number = (base + e).astype(F32).astype(BF16)
                acc = jnp.zeros((rows, rank), BF16)
                for j in range(top):
                    acc = jnp.where(ids[j] == number, hid[:, j * rank : (j + 1) * rank], acc)
                if q < n_src:
                    left[q * n_loc + e] = acc
                else:
                    later_ref[(q - n_src) * n_loc + e] = acc
        own = ids_ref[:, rows_at(x_at * block + at * rows, rows)]
        gates = g_ref[:, at * rows : (at + 1) * rows]
        number = lax.broadcasted_iota(jnp.int32, gates.shape, 0)
        hit = own[0:1, :] == number
        for j in range(1, top):
            hit = hit | (own[j : j + 1, :] == number)
        total = jnp.sum(jnp.where(hit, gates, 0.0), axis=0, keepdims=True)
        total = jnp.broadcast_to(total, gates.shape).T[:, 0:1]
        for h in range(n_piece):
            cols = rows_at(first[h] * half, half)
            acc = total * bias_ref[:, cols]
            for q in range(n_src):
                for e in range(n_loc):
                    w = w_refs[q * n_piece + h][e]
                    acc = acc + jnp.dot(left[q * n_loc + e], w, preferred_element_type=F32)
            out_ref[:, cols] = acc

    return call(
        body,
        [ids_t, bias, gates_t, *hids, *flat_w],
        [((rows, feats), F32), ((later * n_loc, rows, rank), BF16)],
        [pltpu.VMEM((rows, wide), BF16), pltpu.VMEM((n_src * n_loc, rows, rank), BF16)],
    )


def close(x, sums, lefts, wides, pair):
    rows, feats = sums[0].shape
    block = rows * len(sums)
    n_loc = wides[0][0].shape[0]
    n_piece = len(wides[0])
    half = wides[0][0].shape[2]
    flat_w = [w for src in wides for w in src]
    n = len(sums)

    def body(place_ref, x_ref, *refs):
        s_refs, l_refs, w_refs, out_ref = refs[:n], refs[n : 2 * n], refs[2 * n : -1], refs[-1]
        first = [place_ref[0], 1 - place_ref[0]] if pair else [0]
        mine = rows_at(place_ref[1] * block, block)
        for h in range(n_piece):
            cols = rows_at(first[h] * half, half)
            acc = jnp.concatenate([s[:, cols] for s in s_refs], axis=0)
            for q in range(len(wides)):
                for e in range(n_loc):
                    left = jnp.concatenate([r[q * n_loc + e] for r in l_refs], axis=0)
                    w = w_refs[q * n_piece + h][e]
                    acc = acc + jnp.dot(left, w, preferred_element_type=F32)
            xs = x_ref[mine, cols].astype(F32)
            out_ref[:, cols] = (xs + xs * acc).astype(BF16)

    args = [x, *sums, *lefts, *flat_w]
    return call(body, args, [((block, feats), BF16)])[0]


def on_device(
    nb, ne, nz, inputs, expert_ids, gate_weight, reduce_weight, middle_weight, expand_weight, bias
):
    tok, _ = inputs.shape
    n_loc = reduce_weight.shape[0]
    block = tok // ne
    n_row = block // SPLIT
    pair = nb == 2
    ids_t = expert_ids.T

    def swap(w):
        return lax.ppermute(w, "batch", [(0, 1), (1, 0)])

    def whole(w):
        return lax.all_gather(w, "batch", axis=1, tiled=True)

    if pair:
        pieces = [reduce_weight, swap(reduce_weight)]
    else:
        pieces = [whole(reduce_weight)]
        middle_weight, expand_weight = whole(middle_weight), whole(expand_weight)
    far = list(range(1, ne))
    begun = begin()
    gate_t = gate_weight.T
    mids = [middle_weight] + [send(middle_weight, "expert", m, ne) for m in far]
    own, parts, logits = [], [], []
    for h in range(SPLIT):
        logit, mine, *sent = project(inputs, pieces, gate_t, begun, h, n_row, ne, pair)
        own.append(mine)
        logits.append(logit)
        parts.append([send(s, "expert", m, ne) for s, m in zip(sent, far)])
    wide = widen(expand_weight)
    wides = [wide] + [send(wide, "expert", m, ne) for m in far]
    mids = [turn(mids)]
    if pair:
        mids.append(swap(mids[0]))

    sums = []
    for h in range(SPLIT):
        packed = pack(
            ids_t, [own[h]] + parts[h], h, ne, nz, n_loc, logits if h == 0 else ()
        )
        sums.append([packed[0]] + [send(packed[m], "dim", m, nz) for m in range(1, nz)])
    hids, gates_t = [], None
    for h in range(SPLIT):
        hid, *made = mix(ids_t, gates_t, sums[h], mids, h, block, ne, nz, pair)
        gates_t = made[0] if made else gates_t
        hids.append([hid] + [send(hid, "dim", m, nz) for m in range(1, nz)])
    wides = [[w] + ([swap(w)] if pair else []) for w in wides]
    n_src = (ne + 1) // 2
    sums, lefts = [], []
    for h in range(SPLIT):
        total, left = expand(
            inputs, ids_t, bias[None, :], gates_t, hids[h], wides[:n_src], h, ne, nz, n_loc, pair
        )
        sums.append(total)
        lefts.append(left)
    return close(inputs, sums, lefts, wides[n_src:], pair)


def solution(mesh):
    sizes = dict(mesh.shape)
    in_specs = (
        P("batch", "dim"),
        P("batch", None),
        P("dim", None),
        P("expert", ("dim", "batch"), None),
        P("expert", "batch", None),
        P("expert", ("dim", "batch"), None),
        P("dim"),
    )
    out_specs = P(("batch", "expert"), "dim")
    nb, ne, nz = sizes["batch"], sizes["expert"], sizes["dim"]

    def body(*args):
        return on_device(nb, ne, nz, *args)

    return jax.shard_map(body, mesh=mesh, in_specs=in_specs, out_specs=out_specs, check_vma=False)
```

```python
import jax
import jax.numpy as jnp
from jax import lax
from jax.experimental import pallas as pl
from jax.experimental.pallas import tpu as pltpu
from jax.sharding import PartitionSpec as P


F32 = jnp.float32
BF16 = jnp.bfloat16
LAST = (((1,), (1,)), ((), ()))
MIB = 1 << 20
LANES = 128
SPLIT = 2


def peer_to(i, m, n):
    return i ^ m if n & (n - 1) == 0 else (i + m) % n


def peer_from(i, m, n):
    return i ^ m if n & (n - 1) == 0 else (i - m + n) % n


def send(x, axis, m, n):
    return lax.ppermute(x, axis, [(i, peer_to(i, m, n)) for i in range(n)])


def vmem():
    return pl.BlockSpec(memory_space=pltpu.VMEM)


def call(body, args, outs, scratch=(), limit=12, flops=None, held=(), alias=None):
    space = lambda k: pl.BlockSpec(memory_space=pl.ANY) if k in held else vmem()
    cost = None if flops is None else pl.CostEstimate(flops, 0, flops // 500)

    def placed(*refs):
        body([lax.axis_index(a) for a in ("batch", "expert", "dim")], *refs)

    return pl.pallas_call(
        placed,
        in_specs=[space(k) for k in range(len(args))],
        out_specs=[space("out") for _ in outs],
        out_shape=[jax.ShapeDtypeStruct(s, t) for s, t in outs],
        scratch_shapes=list(scratch),
        input_output_aliases={} if alias is None else {alias: 0},
        cost_estimate=cost,
        compiler_params=pltpu.CompilerParams(vmem_limit_bytes=limit * MIB),
    )(*args)


def rows_at(start, size):
    return pl.ds(pl.multiple_of(start, size), size)


def as_rows(cols_t):
    top, n = cols_t.shape
    pad = jnp.zeros((8 - top, n), cols_t.dtype)
    return jnp.concatenate([cols_t, pad], axis=0).T


def begin():
    def body(place_ref, out_ref):
        out_ref[...] = jnp.zeros(out_ref.shape, jnp.int32)

    return call(body, [], [((8, 128), jnp.int32)], flops=6_000_000_000)[0]


def project(x, pieces, gate_t, begun, h, n_row, n_expert, pair):
    n_loc, width, rank = pieces[0].shape
    n_piece = len(pieces)
    block = n_row * SPLIT

    def body(place_ref, x_ref, *refs):
        w_refs, g_ref = refs[:n_piece], refs[n_piece]
        logit_ref, *outs = refs[n_piece + 2 :]
        first = [place_ref[0], 1 - place_ref[0]] if pair else [0]
        starts = [
            peer_to(place_ref[1], m, n_expert) * block + h * n_row for m in range(n_expert)
        ]
        xs = []
        for p in range(n_piece):
            cols = rows_at(first[p] * width, width)
            xs.append(jnp.concatenate([x_ref[rows_at(s, n_row), cols] for s in starts], axis=0))
        for e in range(n_loc):
            acc = jnp.dot(xs[0], w_refs[0][e], preferred_element_type=F32)
            for p in range(1, n_piece):
                acc = acc + jnp.dot(xs[p], w_refs[p][e], preferred_element_type=F32)
            acc = acc.astype(BF16)
            for m in range(n_expert):
                outs[m][:, e * rank : (e + 1) * rank] = acc[m * n_row : (m + 1) * n_row]
        logit = None
        for p in range(n_piece):
            gate = g_ref[:, rows_at(first[p] * width, width)]
            part = lax.dot_general(gate, xs[p][:n_row], LAST, preferred_element_type=F32)
            logit = part if logit is None else logit + part
        logit_ref[...] = logit

    return call(
        body,
        [x, *pieces, gate_t, begun],
        [((gate_t.shape[0], n_row), F32)] + [((n_row, n_loc * rank), BF16)] * n_expert,
        flops=3_000_000_000,
    )


def widen(wide):
    n_loc, half, rank = wide.shape

    def body(place_ref, w_ref, out_ref):
        for e in range(n_loc):
            out_ref[e] = w_ref[e].T

    return call(body, [wide], [((n_loc, rank, half), BF16)])[0]


def turn(mids):
    n_loc, half, rank = mids[0].shape

    def body(place_ref, *refs):
        for q in range(len(mids)):
            for e in range(n_loc):
                refs[-1][q * n_loc + e] = refs[q][e].T

    return call(body, [*mids], [((len(mids) * n_loc, rank, half), BF16)])[0]


def wide_ids(ids_ref, start, n, width):
    ids = as_rows(ids_ref[:, rows_at(start, n)].astype(F32))
    top = ids_ref.shape[0]
    return [jnp.broadcast_to(ids[:, j : j + 1], (n, width)).astype(BF16) for j in range(top)]


def pack(ids_t, parts, at, n_expert, n_dim, n_loc, logits=()):
    rows, wide = parts[0].shape
    rank = wide // n_loc
    per = rows // n_dim
    top = ids_t.shape[0]
    n_part = len(parts)
    n_log = len(logits)
    high_at = sum(l.shape[1] for l in logits)
    deep = logits[0].shape[0] if logits else 0
    more = -(-2 * high_at * deep // (per * LANES)) * LANES

    def body(place_ref, ids_ref, *refs):
        p_refs, scratch = refs[:n_part], refs[-1]
        l_refs, outs = refs[n_part : n_part + n_log], refs[n_part + n_log : -1]
        x_at, z_at = place_ref[1], place_ref[2]
        ids = wide_ids(ids_ref, x_at * (rows * SPLIT) + at * rows, rows, rank)
        for j in range(top):
            acc = jnp.zeros((rows, rank), BF16)
            for q in range(n_part):
                base = peer_from(x_at, q, n_expert) * n_loc
                for e in range(n_loc):
                    number = (base + e).astype(F32).astype(BF16)
                    acc = jnp.where(
                        ids[j] == number, p_refs[q][:, e * rank : (e + 1) * rank], acc
                    )
            scratch[:, j * rank : (j + 1) * rank] = acc
        for m in range(n_dim):
            outs[m][:, : top * rank] = scratch[rows_at(peer_to(z_at, m, n_dim) * per, per), :]
        if logits:
            full = jnp.concatenate([r[...] for r in l_refs], axis=1)
            n = full.shape[1]
            high = full.astype(BF16)
            low = (full - high.astype(F32)).astype(BF16)
            both = jnp.concatenate([high, low], axis=1)
            for m in range(n_dim):
                outs[m][:, top * rank :] = jnp.zeros((per, more), BF16)
                for k, col in enumerate(range(0, 2 * n, LANES)):
                    row, lane = k * deep % per, top * rank + k * deep // per * LANES
                    outs[m][row : row + deep, lane : lane + LANES] = both[:, col : col + LANES]

    return call(
        body,
        [ids_t, *parts, *logits],
        [((per, top * rank + more), BF16)] * n_dim,
        [pltpu.VMEM((rows, top * rank), BF16)],
    )


def mix(ids_t, gates_t, parts, mids, at, block, n_expert, n_dim, pair):
    top, _ = ids_t.shape
    rank = mids[0].shape[1]
    wide = top * rank
    per = block // SPLIT // n_dim
    n_part = len(parts)
    n_piece = len(mids)
    n_all, _, half = mids[0].shape
    n_loc = n_all // n_expert
    make = gates_t is None

    def body(place_ref, ids_ref, *refs):
        if make:
            p_refs, refs = refs[:n_part], refs[n_part:]
        else:
            g_ref, p_refs, refs = refs[0], refs[1 : n_part + 1], refs[n_part + 1 :]
        m_refs, refs = refs[:n_piece], refs[n_piece:]
        if make:
            out_ref, g_out, squash, ids_s, gate_s = refs
            logit = jnp.zeros((n_all, block), F32)
            for p in range(n_part):
                found = []
                for k in range(2 * block // LANES):
                    row, lane = k * n_all % per, wide + k * n_all // per * LANES
                    found.append(p_refs[p][row : row + n_all, lane : lane + LANES].astype(F32))
                found = jnp.concatenate(found, axis=1)
                logit = logit + found[:, :block] + found[:, block:]
            gates_t = jax.nn.sigmoid(logit)
            g_out[...] = gates_t
        else:
            out_ref, squash, ids_s, gate_s = refs
            gates_t = g_ref[...]
        x_at, z_at = place_ref[1], place_ref[2]
        first = [place_ref[0], 1 - place_ref[0]] if pair else [0]
        ids_s[...] = as_rows(ids_ref[:, rows_at(x_at * block, block)])
        gate_s[...] = gates_t.T
        mine = rows_at(at * per * n_dim + z_at * per, per)
        ids, gates = ids_s[mine, :], gate_s[mine, :]
        lane = lax.broadcasted_iota(jnp.int32, gates.shape, 1)
        chosen, gate = [], []
        for j in range(top):
            cols = slice(j * rank, (j + 1) * rank)
            acc = p_refs[0][:per, cols].astype(F32)
            for p in range(1, n_part):
                acc = acc + p_refs[p][:per, cols].astype(F32)
            squash[j * per : (j + 1) * per, :] = jnp.tanh(acc).astype(BF16)
            own = ids[:, j : j + 1]
            chosen.append(own)
            gate.append(jnp.sum(jnp.where(lane == own, gates, 0.0), axis=1, keepdims=True))
        chosen = jnp.broadcast_to(jnp.concatenate(chosen, axis=0), (top * per, half))
        sq = squash[...]
        for h in range(n_piece):
            acc = jnp.zeros((top * per, half), F32)
            for q in range(n_expert):
                base = peer_from(x_at, q, n_expert) * n_loc
                for e in range(n_loc):
                    got = jnp.dot(sq, m_refs[h][q * n_loc + e], preferred_element_type=F32)
                    acc = jnp.where(chosen == base + e, got, acc)
            hid = jnp.tanh(acc)
            for j in range(top):
                start = pl.multiple_of(j * rank + first[h] * half, half)
                gated = hid[j * per : (j + 1) * per, :] * gate[j]
                out_ref[:, pl.ds(start, half)] = gated.astype(BF16)

    return call(
        body,
        [ids_t] + ([] if make else [gates_t]) + [*parts, *mids],
        [((per, wide), BF16)] + ([((n_all, block), F32)] if make else []),
        [
            pltpu.VMEM((top * per, rank), BF16),
            pltpu.VMEM((block, 8), jnp.int32),
            pltpu.VMEM((block, n_all), F32),
        ],
    )


def expand(x, ids_t, bias, gates_t, hids, wides, at, n_expert, n_dim, n_loc, pair):
    per, wide = hids[0].shape
    top, _ = ids_t.shape
    rank = wide // top
    rows = per * n_dim
    block = rows * SPLIT
    feats = x.shape[1]
    n_src = len(wides)
    n_piece = len(wides[0])
    half = wides[0][0].shape[2]
    flat_w = [w for src in wides for w in src]
    n_h, n_w = len(hids), len(flat_w)
    later = n_expert - n_src

    def body(place_ref, ids_ref, bias_ref, g_ref, *refs):
        h_refs, w_refs = refs[:n_h], refs[n_h : n_h + n_w]
        out_ref, later_ref, hid, left = refs[n_h + n_w :]
        x_at, z_at = place_ref[1], place_ref[2]
        first = [place_ref[0], 1 - place_ref[0]] if pair else [0]
        for m in range(n_dim):
            hid[rows_at(peer_from(z_at, m, n_dim) * per, per), :] = h_refs[m][...]
        ids = wide_ids(ids_ref, x_at * block + at * rows, rows, rank)
        for q in range(n_expert):
            base = peer_from(x_at, q, n_expert) * n_loc
            for e in range(n_loc):
                number = (base + e).astype(F32).astype(BF16)
                acc = jnp.zeros((rows, rank), BF16)
                for j in range(top):
                    acc = jnp.where(ids[j] == number, hid[:, j * rank : (j + 1) * rank], acc)
                if q < n_src:
                    left[q * n_loc + e] = acc
                else:
                    later_ref[(q - n_src) * n_loc + e] = acc
        own = ids_ref[:, rows_at(x_at * block + at * rows, rows)]
        gates = g_ref[:, at * rows : (at + 1) * rows]
        number = lax.broadcasted_iota(jnp.int32, gates.shape, 0)
        hit = own[0:1, :] == number
        for j in range(1, top):
            hit = hit | (own[j : j + 1, :] == number)
        total = jnp.sum(jnp.where(hit, gates, 0.0), axis=0, keepdims=True)
        total = jnp.broadcast_to(total, gates.shape).T[:, 0:1]
        for h in range(n_piece):
            cols = rows_at(first[h] * half, half)
            acc = total * bias_ref[:, cols]
            for q in range(n_src):
                for e in range(n_loc):
                    w = w_refs[q * n_piece + h][e]
                    acc = acc + jnp.dot(left[q * n_loc + e], w, preferred_element_type=F32)
            out_ref[:, cols] = acc

    return call(
        body,
        [ids_t, bias, gates_t, *hids, *flat_w],
        [((rows, feats), F32), ((later * n_loc, rows, rank), BF16)],
        [pltpu.VMEM((rows, wide), BF16), pltpu.VMEM((n_src * n_loc, rows, rank), BF16)],
    )


def close(x, sums, lefts, wides, piece, so_far, pair):
    rows, feats = sums[0].shape
    block = rows * len(sums)
    n_loc, _, half = wides[0].shape
    n = len(sums)
    n_w = len(wides)
    n_first = 0 if so_far is None else 1

    def body(place_ref, *refs):
        refs = refs[n_first:]
        x_ref, s_refs, l_refs = refs[0], refs[1 : n + 1], refs[n + 1 : 2 * n + 1]
        w_refs = refs[2 * n + 1 : 2 * n + 1 + n_w]
        out_ref, buf, sem = refs[2 * n + 1 + n_w :]
        first = [place_ref[0], 1 - place_ref[0]] if pair else [0]
        mine = rows_at(place_ref[1] * block, block)
        copies = []
        for c in range(2):
            cut = slice(c * half // 2, (c + 1) * half // 2)
            cols = rows_at(first[piece] * half + c * (half // 2), half // 2)
            acc = jnp.concatenate([s[:, cols] for s in s_refs], axis=0)
            for q in range(n_w):
                for e in range(n_loc):
                    left = jnp.concatenate([r[q * n_loc + e] for r in l_refs], axis=0)
                    acc = acc + jnp.dot(left, w_refs[q][e, :, cut], preferred_element_type=F32)
            xs = x_ref[mine, cols].astype(F32)
            buf[:, cut] = (xs + xs * acc).astype(BF16)
            copies.append(pltpu.make_async_copy(buf.at[:, cut], out_ref.at[:, cols], sem.at[c]))
            copies[-1].start()
        for c in copies:
            c.wait()

    args = ([] if so_far is None else [so_far]) + [x, *sums, *lefts, *wides]
    return call(
        body,
        args,
        [((block, feats), BF16)],
        [pltpu.VMEM((block, half), BF16), pltpu.SemaphoreType.DMA((2,))],
        held=("out",) if so_far is None else ("out", 0),
        alias=None if so_far is None else 0,
    )[0]


def on_device(
    nb, ne, nz, inputs, expert_ids, gate_weight, reduce_weight, middle_weight, expand_weight, bias
):
    tok, _ = inputs.shape
    n_loc = reduce_weight.shape[0]
    block = tok // ne
    n_row = block // SPLIT
    pair = nb == 2
    ids_t = expert_ids.T

    def swap(w):
        return lax.ppermute(w, "batch", [(0, 1), (1, 0)])

    def whole(w):
        return lax.all_gather(w, "batch", axis=1, tiled=True)

    if pair:
        pieces = [reduce_weight, swap(reduce_weight)]
    else:
        pieces = [whole(reduce_weight)]
        middle_weight, expand_weight = whole(middle_weight), whole(expand_weight)
    far = list(range(1, ne))
    begun = begin()
    gate_t = gate_weight.T
    mids = [middle_weight] + [send(middle_weight, "expert", m, ne) for m in far]
    own, parts, logits = [], [], []
    for h in range(SPLIT):
        logit, mine, *sent = project(inputs, pieces, gate_t, begun, h, n_row, ne, pair)
        own.append(mine)
        logits.append(logit)
        parts.append([send(s, "expert", m, ne) for s, m in zip(sent, far)])
    wide = widen(expand_weight)
    wides = [wide] + [send(wide, "expert", m, ne) for m in far]
    mids = [turn(mids)]
    if pair:
        mids.append(swap(mids[0]))

    sums = []
    for h in range(SPLIT):
        packed = pack(
            ids_t, [own[h]] + parts[h], h, ne, nz, n_loc, logits if h == 0 else ()
        )
        sums.append([packed[0]] + [send(packed[m], "dim", m, nz) for m in range(1, nz)])
    hids, gates_t = [], None
    for h in range(SPLIT):
        hid, *made = mix(ids_t, gates_t, sums[h], mids, h, block, ne, nz, pair)
        gates_t = made[0] if made else gates_t
        hids.append([hid] + [send(hid, "dim", m, nz) for m in range(1, nz)])
    wides = [[w] + ([swap(w)] if pair else []) for w in wides]
    n_src = max(1, ne - 1)
    sums, lefts = [], []
    for h in range(SPLIT):
        total, left = expand(
            inputs, ids_t, bias[None, :], gates_t, hids[h], wides[:n_src], h, ne, nz, n_loc, pair
        )
        sums.append(total)
        lefts.append(left)
    out = None
    for k in range(len(wides[0])):
        out = close(inputs, sums, lefts, [w[k] for w in wides[n_src:]], k, out, pair)
    return out


def solution(mesh):
    sizes = dict(mesh.shape)
    in_specs = (
        P("batch", "dim"),
        P("batch", None),
        P("dim", None),
        P("expert", ("dim", "batch"), None),
        P("expert", "batch", None),
        P("expert", ("dim", "batch"), None),
        P("dim"),
    )
    out_specs = P(("batch", "expert"), "dim")
    nb, ne, nz = sizes["batch"], sizes["expert"], sizes["dim"]

    def body(*args):
        return on_device(nb, ne, nz, *args)

    return jax.shard_map(body, mesh=mesh, in_specs=in_specs, out_specs=out_specs, check_vma=False)
```

```python
import jax
import jax.numpy as jnp
from jax import lax
from jax.experimental import pallas as pl
from jax.experimental.pallas import tpu as pltpu
from jax.sharding import PartitionSpec as P


F32 = jnp.float32
BF16 = jnp.bfloat16
LAST = (((1,), (1,)), ((), ()))
MIB = 1 << 20
LANES = 128
SPLIT = 2


def peer_to(i, m, n):
    return i ^ m if n & (n - 1) == 0 else (i + m) % n


def peer_from(i, m, n):
    return i ^ m if n & (n - 1) == 0 else (i - m + n) % n


def send(x, axis, m, n):
    return lax.ppermute(x, axis, [(i, peer_to(i, m, n)) for i in range(n)])


def vmem():
    return pl.BlockSpec(memory_space=pltpu.VMEM)


def call(body, args, outs, scratch=(), limit=12, flops=None, held=(), alias=None):
    space = lambda k: pl.BlockSpec(memory_space=pl.ANY) if k in held else vmem()
    cost = None if flops is None else pl.CostEstimate(flops, 0, flops // 500)

    def placed(*refs):
        body([lax.axis_index(a) for a in ("batch", "expert", "dim")], *refs)

    return pl.pallas_call(
        placed,
        in_specs=[space(k) for k in range(len(args))],
        out_specs=[space("out") for _ in outs],
        out_shape=[jax.ShapeDtypeStruct(s, t) for s, t in outs],
        scratch_shapes=list(scratch),
        input_output_aliases={} if alias is None else {alias: 0},
        cost_estimate=cost,
        compiler_params=pltpu.CompilerParams(vmem_limit_bytes=limit * MIB),
    )(*args)


def rows_at(start, size):
    return pl.ds(pl.multiple_of(start, size), size)


def as_rows(cols_t):
    top, n = cols_t.shape
    pad = jnp.zeros((8 - top, n), cols_t.dtype)
    return jnp.concatenate([cols_t, pad], axis=0).T


def begin():
    def body(place_ref, out_ref):
        out_ref[...] = jnp.zeros(out_ref.shape, jnp.int32)

    return call(body, [], [((8, 128), jnp.int32)], flops=6_000_000_000)[0]


def project(x, pieces, gate_t, begun, h, n_row, n_expert, pair, relayed=()):
    n_loc, width, rank = pieces[0].shape
    n_piece = len(pieces)
    n_relay = len(relayed)
    more = {m: mid.shape[1] // n_loc for m, mid in relayed}
    block = n_row * SPLIT

    def body(place_ref, x_ref, *refs):
        w_refs, g_ref = refs[:n_piece], refs[n_piece]
        mid_refs = refs[n_piece + 2 : n_piece + 2 + n_relay]
        logit_ref, *outs = refs[n_piece + 2 + n_relay :]
        for (m, _), mid_ref in zip(relayed, mid_refs):
            for k, e in enumerate(relayed_by(m, n_loc)):
                at = n_row + k * more[m]
                for c in range(n_loc):
                    outs[m][at : at + more[m], c * rank : (c + 1) * rank] = mid_ref[
                        e, c * more[m] : (c + 1) * more[m], :
                    ]
        first = [place_ref[0], 1 - place_ref[0]] if pair else [0]
        starts = [
            peer_to(place_ref[1], m, n_expert) * block + h * n_row for m in range(n_expert)
        ]
        xs = []
        for p in range(n_piece):
            cols = rows_at(first[p] * width, width)
            xs.append(jnp.concatenate([x_ref[rows_at(s, n_row), cols] for s in starts], axis=0))
        for e in range(n_loc):
            acc = jnp.dot(xs[0], w_refs[0][e], preferred_element_type=F32)
            for p in range(1, n_piece):
                acc = acc + jnp.dot(xs[p], w_refs[p][e], preferred_element_type=F32)
            acc = acc.astype(BF16)
            for m in range(n_expert):
                outs[m][:n_row, e * rank : (e + 1) * rank] = acc[m * n_row : (m + 1) * n_row]
        logit = None
        for p in range(n_piece):
            gate = g_ref[:, rows_at(first[p] * width, width)]
            part = lax.dot_general(gate, xs[p][:n_row], LAST, preferred_element_type=F32)
            logit = part if logit is None else logit + part
        logit_ref[...] = logit

    return call(
        body,
        [x, *pieces, gate_t, begun] + [mid for _, mid in relayed],
        [((gate_t.shape[0], n_row), F32)]
        + [
            ((n_row + more.get(m, 0) * len(relayed_by(m, n_loc)), n_loc * rank), BF16)
            for m in range(n_expert)
        ],
        flops=3_000_000_000,
    )


def widen(wide):
    n_loc, half, rank = wide.shape

    def body(place_ref, w_ref, out_ref):
        for e in range(n_loc):
            out_ref[e] = w_ref[e].T

    return call(body, [wide], [((n_loc, rank, half), BF16)])[0]


def turn(mids, relayed, n_row):
    n_loc, half, rank = mids[0].shape
    n = len(mids)
    more = half // n_loc

    def body(place_ref, *refs):
        out_ref = refs[-1]
        for q in range(n):
            for e in range(n_loc):
                out_ref[q * n_loc + e] = refs[q][e].T
        for m in range(1, len(relayed) + 1):
            part = refs[n + m - 1]
            for k, e in enumerate(relayed_by(m, n_loc)):
                at = n_row + k * more
                rows = [part[at : at + more, c * rank : (c + 1) * rank] for c in range(n_loc)]
                out_ref[n * n_loc + e] = jnp.concatenate(rows, axis=0).T

    count = n * n_loc + (n_loc if relayed else 0)
    return call(body, [*mids, *relayed], [((count, rank, half), BF16)])[0]


def wide_ids(ids_ref, start, n, width):
    ids = as_rows(ids_ref[:, rows_at(start, n)].astype(F32))
    top = ids_ref.shape[0]
    return [jnp.broadcast_to(ids[:, j : j + 1], (n, width)).astype(BF16) for j in range(top)]


def pack(ids_t, parts, at, n_expert, n_dim, n_loc, logits=()):
    rows, wide = parts[0].shape
    rank = wide // n_loc
    per = rows // n_dim
    top = ids_t.shape[0]
    n_part = len(parts)
    n_log = len(logits)
    high_at = sum(l.shape[1] for l in logits)
    deep = logits[0].shape[0] if logits else 0
    more = -(-2 * high_at * deep // (per * LANES)) * LANES

    def body(place_ref, ids_ref, *refs):
        p_refs, scratch = refs[:n_part], refs[-1]
        l_refs, outs = refs[n_part : n_part + n_log], refs[n_part + n_log : -1]
        x_at, z_at = place_ref[1], place_ref[2]
        ids = wide_ids(ids_ref, x_at * (rows * SPLIT) + at * rows, rows, rank)
        for j in range(top):
            acc = jnp.zeros((rows, rank), BF16)
            for q in range(n_part):
                base = peer_from(x_at, q, n_expert) * n_loc
                for e in range(n_loc):
                    number = (base + e).astype(F32).astype(BF16)
                    acc = jnp.where(
                        ids[j] == number, p_refs[q][:rows, e * rank : (e + 1) * rank], acc
                    )
            scratch[:, j * rank : (j + 1) * rank] = acc
        for m in range(n_dim):
            outs[m][:, : top * rank] = scratch[rows_at(peer_to(z_at, m, n_dim) * per, per), :]
        if logits:
            full = jnp.concatenate([r[...] for r in l_refs], axis=1)
            n = full.shape[1]
            high = full.astype(BF16)
            low = (full - high.astype(F32)).astype(BF16)
            both = jnp.concatenate([high, low], axis=1)
            for m in range(n_dim):
                outs[m][:, top * rank :] = jnp.zeros((per, more), BF16)
                for k, col in enumerate(range(0, 2 * n, LANES)):
                    row, lane = k * deep % per, top * rank + k * deep // per * LANES
                    outs[m][row : row + deep, lane : lane + LANES] = both[:, col : col + LANES]

    return call(
        body,
        [ids_t, *parts, *logits],
        [((per, top * rank + more), BF16)] * n_dim,
        [pltpu.VMEM((rows, top * rank), BF16)],
    )


def mix(ids_t, gates_t, parts, mids, at, block, n_expert, n_dim, pair):
    top, _ = ids_t.shape
    rank = mids[0].shape[1]
    wide = top * rank
    per = block // SPLIT // n_dim
    n_part = len(parts)
    n_piece = len(mids)
    n_all, _, half = mids[0].shape
    n_loc = n_all // n_expert
    make = gates_t is None

    def body(place_ref, ids_ref, *refs):
        if make:
            p_refs, refs = refs[:n_part], refs[n_part:]
        else:
            g_ref, p_refs, refs = refs[0], refs[1 : n_part + 1], refs[n_part + 1 :]
        m_refs, refs = refs[:n_piece], refs[n_piece:]
        if make:
            out_ref, g_out, squash, ids_s, gate_s = refs
            logit = jnp.zeros((n_all, block), F32)
            for p in range(n_part):
                found = []
                for k in range(2 * block // LANES):
                    row, lane = k * n_all % per, wide + k * n_all // per * LANES
                    found.append(p_refs[p][row : row + n_all, lane : lane + LANES].astype(F32))
                found = jnp.concatenate(found, axis=1)
                logit = logit + found[:, :block] + found[:, block:]
            gates_t = jax.nn.sigmoid(logit)
            g_out[...] = gates_t
        else:
            out_ref, squash, ids_s, gate_s = refs
            gates_t = g_ref[...]
        x_at, z_at = place_ref[1], place_ref[2]
        first = [place_ref[0], 1 - place_ref[0]] if pair else [0]
        ids_s[...] = as_rows(ids_ref[:, rows_at(x_at * block, block)])
        gate_s[...] = gates_t.T
        mine = rows_at(at * per * n_dim + z_at * per, per)
        ids, gates = ids_s[mine, :], gate_s[mine, :]
        lane = lax.broadcasted_iota(jnp.int32, gates.shape, 1)
        chosen, gate = [], []
        for j in range(top):
            cols = slice(j * rank, (j + 1) * rank)
            acc = p_refs[0][:per, cols].astype(F32)
            for p in range(1, n_part):
                acc = acc + p_refs[p][:per, cols].astype(F32)
            squash[j * per : (j + 1) * per, :] = jnp.tanh(acc).astype(BF16)
            own = ids[:, j : j + 1]
            chosen.append(own)
            gate.append(jnp.sum(jnp.where(lane == own, gates, 0.0), axis=1, keepdims=True))
        chosen = jnp.broadcast_to(jnp.concatenate(chosen, axis=0), (top * per, half))
        sq = squash[...]
        for h in range(n_piece):
            acc = jnp.zeros((top * per, half), F32)
            for q in range(n_expert):
                base = peer_from(x_at, q, n_expert) * n_loc
                for e in range(n_loc):
                    got = jnp.dot(sq, m_refs[h][q * n_loc + e], preferred_element_type=F32)
                    acc = jnp.where(chosen == base + e, got, acc)
            hid = jnp.tanh(acc)
            for j in range(top):
                start = pl.multiple_of(j * rank + first[h] * half, half)
                gated = hid[j * per : (j + 1) * per, :] * gate[j]
                out_ref[:, pl.ds(start, half)] = gated.astype(BF16)

    return call(
        body,
        [ids_t] + ([] if make else [gates_t]) + [*parts, *mids],
        [((per, wide), BF16)] + ([((n_all, block), F32)] if make else []),
        [
            pltpu.VMEM((top * per, rank), BF16),
            pltpu.VMEM((block, 8), jnp.int32),
            pltpu.VMEM((block, n_all), F32),
        ],
    )


def expand(x, ids_t, bias, gates_t, hids, wides, at, n_expert, n_dim, n_loc, pair):
    per, wide = hids[0].shape
    top, _ = ids_t.shape
    rank = wide // top
    rows = per * n_dim
    block = rows * SPLIT
    feats = x.shape[1]
    n_src = len(wides)
    n_piece = len(wides[0])
    half = wides[0][0].shape[2]
    flat_w = [w for src in wides for w in src]
    n_h, n_w = len(hids), len(flat_w)
    later = n_expert - n_src

    def body(place_ref, ids_ref, bias_ref, g_ref, *refs):
        h_refs, w_refs = refs[:n_h], refs[n_h : n_h + n_w]
        out_ref, later_ref, hid, left = refs[n_h + n_w :]
        x_at, z_at = place_ref[1], place_ref[2]
        first = [place_ref[0], 1 - place_ref[0]] if pair else [0]
        for m in range(n_dim):
            hid[rows_at(peer_from(z_at, m, n_dim) * per, per), :] = h_refs[m][...]
        ids = wide_ids(ids_ref, x_at * block + at * rows, rows, rank)
        for q in range(n_expert):
            base = peer_from(x_at, q, n_expert) * n_loc
            for e in range(n_loc):
                number = (base + e).astype(F32).astype(BF16)
                acc = jnp.zeros((rows, rank), BF16)
                for j in range(top):
                    acc = jnp.where(ids[j] == number, hid[:, j * rank : (j + 1) * rank], acc)
                if q < n_src:
                    left[q * n_loc + e] = acc
                else:
                    later_ref[(q - n_src) * n_loc + e] = acc
        own = ids_ref[:, rows_at(x_at * block + at * rows, rows)]
        gates = g_ref[:, at * rows : (at + 1) * rows]
        number = lax.broadcasted_iota(jnp.int32, gates.shape, 0)
        hit = own[0:1, :] == number
        for j in range(1, top):
            hit = hit | (own[j : j + 1, :] == number)
        total = jnp.sum(jnp.where(hit, gates, 0.0), axis=0, keepdims=True)
        total = jnp.broadcast_to(total, gates.shape).T[:, 0:1]
        for h in range(n_piece):
            cols = rows_at(first[h] * half, half)
            acc = total * bias_ref[:, cols]
            for q in range(n_src):
                for e in range(n_loc):
                    w = w_refs[q * n_piece + h][e]
                    acc = acc + jnp.dot(left[q * n_loc + e], w, preferred_element_type=F32)
            out_ref[:, cols] = acc

    return call(
        body,
        [ids_t, bias, gates_t, *hids, *flat_w],
        [((rows, feats), F32), ((later * n_loc, rows, rank), BF16)],
        [pltpu.VMEM((rows, wide), BF16), pltpu.VMEM((n_src * n_loc, rows, rank), BF16)],
    )


def close(x, sums, lefts, wides, piece, so_far, pair):
    rows, feats = sums[0].shape
    block = rows * len(sums)
    n_loc, _, half = wides[0].shape
    n = len(sums)
    n_w = len(wides)
    n_first = 0 if so_far is None else 1

    def body(place_ref, *refs):
        refs = refs[n_first:]
        x_ref, s_refs, l_refs = refs[0], refs[1 : n + 1], refs[n + 1 : 2 * n + 1]
        w_refs = refs[2 * n + 1 : 2 * n + 1 + n_w]
        out_ref, buf, sem = refs[2 * n + 1 + n_w :]
        first = [place_ref[0], 1 - place_ref[0]] if pair else [0]
        mine = rows_at(place_ref[1] * block, block)
        copies = []
        for c in range(2):
            cut = slice(c * half // 2, (c + 1) * half // 2)
            cols = rows_at(first[piece] * half + c * (half // 2), half // 2)
            acc = jnp.concatenate([s[:, cols] for s in s_refs], axis=0)
            for q in range(n_w):
                for e in range(n_loc):
                    left = jnp.concatenate([r[q * n_loc + e] for r in l_refs], axis=0)
                    acc = acc + jnp.dot(left, w_refs[q][e, :, cut], preferred_element_type=F32)
            xs = x_ref[mine, cols].astype(F32)
            buf[:, cut] = (xs + xs * acc).astype(BF16)
            copies.append(pltpu.make_async_copy(buf.at[:, cut], out_ref.at[:, cols], sem.at[c]))
            copies[-1].start()
        for c in copies:
            c.wait()

    args = ([] if so_far is None else [so_far]) + [x, *sums, *lefts, *wides]
    return call(
        body,
        args,
        [((block, feats), BF16)],
        [pltpu.VMEM((block, half), BF16), pltpu.SemaphoreType.DMA((2,))],
        held=("out",) if so_far is None else ("out", 0),
        alias=None if so_far is None else 0,
    )[0]


def relays(ne):
    return ne == 4


def relayed_by(m, n_loc):
    return [e for e in range(n_loc) if e % 2 == m - 1]


def on_device(
    nb, ne, nz, inputs, expert_ids, gate_weight, reduce_weight, middle_weight, expand_weight, bias
):
    tok, _ = inputs.shape
    n_loc = reduce_weight.shape[0]
    block = tok // ne
    n_row = block // SPLIT
    pair = nb == 2
    ids_t = expert_ids.T

    def swap(w):
        return lax.ppermute(w, "batch", [(0, 1), (1, 0)])

    def whole(w):
        return lax.all_gather(w, "batch", axis=1, tiled=True)

    if pair:
        pieces = [reduce_weight, swap(reduce_weight)]
    else:
        pieces = [whole(reduce_weight)]
        middle_weight, expand_weight = whole(middle_weight), whole(expand_weight)
    far = list(range(1, ne))
    begun = begin()
    gate_t = gate_weight.T
    near = far[:-1] if relays(ne) else far
    mids = [middle_weight] + [send(middle_weight, "expert", m, ne) for m in near]
    own, parts, logits = [], [], []
    for h in range(SPLIT):
        last = h == SPLIT - 1 and relays(ne)
        logit, mine, *sent = project(
            inputs, pieces, gate_t, begun, h, n_row, ne, pair,
            [(m, mids[ne - 1 - m]) for m in near] if last else (),
        )
        own.append(mine)
        logits.append(logit)
        parts.append([send(s, "expert", m, ne) for s, m in zip(sent, far)])
    wide = widen(expand_weight)
    wides = [wide] + [send(wide, "expert", m, ne) for m in far]
    mids = [turn(mids, parts[-1][: len(near)] if relays(ne) else [], n_row)]
    if pair:
        mids.append(swap(mids[0]))

    sums = []
    for h in range(SPLIT):
        packed = pack(
            ids_t, [own[h]] + parts[h], h, ne, nz, n_loc, logits if h == 0 else ()
        )
        sums.append([packed[0]] + [send(packed[m], "dim", m, nz) for m in range(1, nz)])
    hids, gates_t = [], None
    for h in range(SPLIT):
        hid, *made = mix(ids_t, gates_t, sums[h], mids, h, block, ne, nz, pair)
        gates_t = made[0] if made else gates_t
        hids.append([hid] + [send(hid, "dim", m, nz) for m in range(1, nz)])
    wides = [[w] + ([swap(w)] if pair else []) for w in wides]
    n_src = (ne + 1) // 2
    sums, lefts = [], []
    for h in range(SPLIT):
        total, left = expand(
            inputs, ids_t, bias[None, :], gates_t, hids[h], wides[:n_src], h, ne, nz, n_loc, pair
        )
        sums.append(total)
        lefts.append(left)
    out = None
    for k in range(len(wides[0])):
        out = close(inputs, sums, lefts, [w[k] for w in wides[n_src:]], k, out, pair)
    return out


def solution(mesh):
    sizes = dict(mesh.shape)
    in_specs = (
        P("batch", "dim"),
        P("batch", None),
        P("dim", None),
        P("expert", ("dim", "batch"), None),
        P("expert", "batch", None),
        P("expert", ("dim", "batch"), None),
        P("dim"),
    )
    out_specs = P(("batch", "expert"), "dim")
    nb, ne, nz = sizes["batch"], sizes["expert"], sizes["dim"]

    def body(*args):
        return on_device(nb, ne, nz, *args)

    return jax.shard_map(body, mesh=mesh, in_specs=in_specs, out_specs=out_specs, check_vma=False)
```

```python
import jax
import jax.numpy as jnp
from jax import lax
from jax.experimental import pallas as pl
from jax.experimental.pallas import tpu as pltpu
from jax.sharding import PartitionSpec as P


F32 = jnp.float32
BF16 = jnp.bfloat16
LAST = (((1,), (1,)), ((), ()))
MIB = 1 << 20
LANES = 128
SPLIT = 2


def peer_to(i, m, n):
    return i ^ m if n & (n - 1) == 0 else (i + m) % n


def peer_from(i, m, n):
    return i ^ m if n & (n - 1) == 0 else (i - m + n) % n


def send(x, axis, m, n):
    return lax.ppermute(x, axis, [(i, peer_to(i, m, n)) for i in range(n)])


def vmem():
    return pl.BlockSpec(memory_space=pltpu.VMEM)


def call(body, args, outs, scratch=(), limit=12, flops=None, held=(), alias=None):
    space = lambda k: pl.BlockSpec(memory_space=pl.ANY) if k in held else vmem()
    cost = None if flops is None else pl.CostEstimate(flops, 0, flops // 500)

    def placed(*refs):
        body([lax.axis_index(a) for a in ("batch", "expert", "dim")], *refs)

    return pl.pallas_call(
        placed,
        in_specs=[space(k) for k in range(len(args))],
        out_specs=[space("out") for _ in outs],
        out_shape=[jax.ShapeDtypeStruct(s, t) for s, t in outs],
        scratch_shapes=list(scratch),
        input_output_aliases={} if alias is None else {alias: 0},
        cost_estimate=cost,
        compiler_params=pltpu.CompilerParams(vmem_limit_bytes=limit * MIB),
    )(*args)


def rows_at(start, size):
    return pl.ds(pl.multiple_of(start, size), size)


def as_rows(cols_t):
    top, n = cols_t.shape
    pad = jnp.zeros((8 - top, n), cols_t.dtype)
    return jnp.concatenate([cols_t, pad], axis=0).T


def begin():
    def body(place_ref, out_ref):
        out_ref[...] = jnp.zeros(out_ref.shape, jnp.int32)

    return call(body, [], [((8, 128), jnp.int32)], flops=6_000_000_000)[0]


def project(x, pieces, gate_t, begun, h, n_row, n_expert, pair, relayed=()):
    n_loc, width, rank = pieces[0].shape
    n_piece = len(pieces)
    n_relay = len(relayed)
    more = {m: mid.shape[1] // n_loc for m, mid in relayed}
    block = n_row * SPLIT

    def body(place_ref, x_ref, *refs):
        w_refs, g_ref = refs[:n_piece], refs[n_piece]
        mid_refs = refs[n_piece + 2 : n_piece + 2 + n_relay]
        logit_ref, *outs = refs[n_piece + 2 + n_relay :]
        for (m, _), mid_ref in zip(relayed, mid_refs):
            for k, e in enumerate(relayed_by(m, n_loc)):
                at = n_row + k * more[m]
                for c in range(n_loc):
                    outs[m][at : at + more[m], c * rank : (c + 1) * rank] = mid_ref[
                        e, c * more[m] : (c + 1) * more[m], :
                    ]
        first = [place_ref[0], 1 - place_ref[0]] if pair else [0]
        starts = [
            peer_to(place_ref[1], m, n_expert) * block + h * n_row for m in range(n_expert)
        ]
        xs = []
        for p in range(n_piece):
            cols = rows_at(first[p] * width, width)
            xs.append(jnp.concatenate([x_ref[rows_at(s, n_row), cols] for s in starts], axis=0))
        for e in range(n_loc):
            acc = jnp.dot(xs[0], w_refs[0][e], preferred_element_type=F32)
            for p in range(1, n_piece):
                acc = acc + jnp.dot(xs[p], w_refs[p][e], preferred_element_type=F32)
            acc = acc.astype(BF16)
            for m in range(n_expert):
                outs[m][:n_row, e * rank : (e + 1) * rank] = acc[m * n_row : (m + 1) * n_row]
        logit = None
        for p in range(n_piece):
            gate = g_ref[:, rows_at(first[p] * width, width)]
            part = lax.dot_general(gate, xs[p][:n_row], LAST, preferred_element_type=F32)
            logit = part if logit is None else logit + part
        logit_ref[...] = logit

    return call(
        body,
        [x, *pieces, gate_t, begun] + [mid for _, mid in relayed],
        [((gate_t.shape[0], n_row), F32)]
        + [
            ((n_row + more.get(m, 0) * len(relayed_by(m, n_loc)), n_loc * rank), BF16)
            for m in range(n_expert)
        ],
        flops=3_000_000_000,
    )


def widen(wide):
    n_loc, half, rank = wide.shape

    def body(place_ref, w_ref, out_ref):
        for e in range(n_loc):
            out_ref[e] = w_ref[e].T

    return call(body, [wide], [((n_loc, rank, half), BF16)])[0]


def turn(mids, relayed, n_row):
    n_loc, half, rank = mids[0].shape
    n = len(mids)
    more = half // n_loc

    def body(place_ref, *refs):
        out_ref = refs[-1]
        for q in range(n):
            for e in range(n_loc):
                out_ref[q * n_loc + e] = refs[q][e].T
        for m in range(1, len(relayed) + 1):
            part = refs[n + m - 1]
            for k, e in enumerate(relayed_by(m, n_loc)):
                at = n_row + k * more
                rows = [part[at : at + more, c * rank : (c + 1) * rank] for c in range(n_loc)]
                out_ref[n * n_loc + e] = jnp.concatenate(rows, axis=0).T

    count = n * n_loc + (n_loc if relayed else 0)
    return call(body, [*mids, *relayed], [((count, rank, half), BF16)])[0]


def wide_ids(ids_ref, start, n, width):
    ids = as_rows(ids_ref[:, rows_at(start, n)].astype(F32))
    top = ids_ref.shape[0]
    return [jnp.broadcast_to(ids[:, j : j + 1], (n, width)).astype(BF16) for j in range(top)]


def pack(ids_t, parts, at, n_expert, n_dim, n_loc, logits=()):
    rows, wide = parts[0].shape
    rank = wide // n_loc
    per = rows // n_dim
    top = ids_t.shape[0]
    n_part = len(parts)
    n_log = len(logits)
    high_at = sum(l.shape[1] for l in logits)
    deep = logits[0].shape[0] if logits else 0
    more = -(-2 * high_at * deep // (per * LANES)) * LANES

    def body(place_ref, ids_ref, *refs):
        p_refs, scratch = refs[:n_part], refs[-1]
        l_refs, outs = refs[n_part : n_part + n_log], refs[n_part + n_log : -1]
        x_at, z_at = place_ref[1], place_ref[2]
        ids = wide_ids(ids_ref, x_at * (rows * SPLIT) + at * rows, rows, rank)
        for j in range(top):
            acc = jnp.zeros((rows, rank), BF16)
            for q in range(n_part):
                base = peer_from(x_at, q, n_expert) * n_loc
                for e in range(n_loc):
                    number = (base + e).astype(F32).astype(BF16)
                    acc = jnp.where(
                        ids[j] == number, p_refs[q][:rows, e * rank : (e + 1) * rank], acc
                    )
            scratch[:, j * rank : (j + 1) * rank] = acc
        for m in range(n_dim):
            outs[m][:, : top * rank] = scratch[rows_at(peer_to(z_at, m, n_dim) * per, per), :]
        if logits:
            full = jnp.concatenate([r[...] for r in l_refs], axis=1)
            n = full.shape[1]
            high = full.astype(BF16)
            low = (full - high.astype(F32)).astype(BF16)
            both = jnp.concatenate([high, low], axis=1)
            for m in range(n_dim):
                outs[m][:, top * rank :] = jnp.zeros((per, more), BF16)
                for k, col in enumerate(range(0, 2 * n, LANES)):
                    row, lane = k * deep % per, top * rank + k * deep // per * LANES
                    outs[m][row : row + deep, lane : lane + LANES] = both[:, col : col + LANES]

    return call(
        body,
        [ids_t, *parts, *logits],
        [((per, top * rank + more), BF16)] * n_dim,
        [pltpu.VMEM((rows, top * rank), BF16)],
    )


def mix(ids_t, gates_t, parts, mids, at, block, n_expert, n_dim, pair):
    top, _ = ids_t.shape
    rank = mids[0].shape[1]
    wide = top * rank
    per = block // SPLIT // n_dim
    n_part = len(parts)
    n_piece = len(mids)
    n_all, _, half = mids[0].shape
    n_loc = n_all // n_expert
    make = gates_t is None

    def body(place_ref, ids_ref, *refs):
        if make:
            p_refs, refs = refs[:n_part], refs[n_part:]
        else:
            g_ref, p_refs, refs = refs[0], refs[1 : n_part + 1], refs[n_part + 1 :]
        m_refs, refs = refs[:n_piece], refs[n_piece:]
        if make:
            out_ref, g_out, squash, ids_s, gate_s = refs
            logit = jnp.zeros((n_all, block), F32)
            for p in range(n_part):
                found = []
                for k in range(2 * block // LANES):
                    row, lane = k * n_all % per, wide + k * n_all // per * LANES
                    found.append(p_refs[p][row : row + n_all, lane : lane + LANES].astype(F32))
                found = jnp.concatenate(found, axis=1)
                logit = logit + found[:, :block] + found[:, block:]
            gates_t = jax.nn.sigmoid(logit)
            g_out[...] = gates_t
        else:
            out_ref, squash, ids_s, gate_s = refs
            gates_t = g_ref[...]
        x_at, z_at = place_ref[1], place_ref[2]
        first = [place_ref[0], 1 - place_ref[0]] if pair else [0]
        ids_s[...] = as_rows(ids_ref[:, rows_at(x_at * block, block)])
        gate_s[...] = gates_t.T
        mine = rows_at(at * per * n_dim + z_at * per, per)
        ids, gates = ids_s[mine, :], gate_s[mine, :]
        lane = lax.broadcasted_iota(jnp.int32, gates.shape, 1)
        chosen, gate = [], []
        for j in range(top):
            cols = slice(j * rank, (j + 1) * rank)
            acc = p_refs[0][:per, cols].astype(F32)
            for p in range(1, n_part):
                acc = acc + p_refs[p][:per, cols].astype(F32)
            squash[j * per : (j + 1) * per, :] = jnp.tanh(acc).astype(BF16)
            own = ids[:, j : j + 1]
            chosen.append(own)
            gate.append(jnp.sum(jnp.where(lane == own, gates, 0.0), axis=1, keepdims=True))
        chosen = jnp.broadcast_to(jnp.concatenate(chosen, axis=0), (top * per, half))
        sq = squash[...]
        for h in range(n_piece):
            acc = jnp.zeros((top * per, half), F32)
            for q in range(n_expert):
                base = peer_from(x_at, q, n_expert) * n_loc
                for e in range(n_loc):
                    got = jnp.dot(sq, m_refs[h][q * n_loc + e], preferred_element_type=F32)
                    acc = jnp.where(chosen == base + e, got, acc)
            hid = jnp.tanh(acc)
            for j in range(top):
                start = pl.multiple_of(j * rank + first[h] * half, half)
                gated = hid[j * per : (j + 1) * per, :] * gate[j]
                out_ref[:, pl.ds(start, half)] = gated.astype(BF16)

    return call(
        body,
        [ids_t] + ([] if make else [gates_t]) + [*parts, *mids],
        [((per, wide), BF16)] + ([((n_all, block), F32)] if make else []),
        [
            pltpu.VMEM((top * per, rank), BF16),
            pltpu.VMEM((block, 8), jnp.int32),
            pltpu.VMEM((block, n_all), F32),
        ],
    )


def expand(x, ids_t, bias, gates_t, hids, wides, at, n_expert, n_dim, n_loc, pair):
    per, wide = hids[0].shape
    top, _ = ids_t.shape
    rank = wide // top
    rows = per * n_dim
    block = rows * SPLIT
    feats = x.shape[1]
    n_src = len(wides)
    n_piece = len(wides[0])
    half = wides[0][0].shape[2]
    flat_w = [w for src in wides for w in src]
    n_h, n_w = len(hids), len(flat_w)
    later = n_expert - n_src

    def body(place_ref, ids_ref, bias_ref, g_ref, *refs):
        h_refs, w_refs = refs[:n_h], refs[n_h : n_h + n_w]
        out_ref, later_ref, hid, left = refs[n_h + n_w :]
        x_at, z_at = place_ref[1], place_ref[2]
        first = [place_ref[0], 1 - place_ref[0]] if pair else [0]
        for m in range(n_dim):
            hid[rows_at(peer_from(z_at, m, n_dim) * per, per), :] = h_refs[m][...]
        ids = wide_ids(ids_ref, x_at * block + at * rows, rows, rank)
        for q in range(n_expert):
            base = peer_from(x_at, q, n_expert) * n_loc
            for e in range(n_loc):
                number = (base + e).astype(F32).astype(BF16)
                acc = jnp.zeros((rows, rank), BF16)
                for j in range(top):
                    acc = jnp.where(ids[j] == number, hid[:, j * rank : (j + 1) * rank], acc)
                if q < n_src:
                    left[q * n_loc + e] = acc
                else:
                    later_ref[(q - n_src) * n_loc + e] = acc
        own = ids_ref[:, rows_at(x_at * block + at * rows, rows)]
        gates = g_ref[:, at * rows : (at + 1) * rows]
        number = lax.broadcasted_iota(jnp.int32, gates.shape, 0)
        hit = own[0:1, :] == number
        for j in range(1, top):
            hit = hit | (own[j : j + 1, :] == number)
        total = jnp.sum(jnp.where(hit, gates, 0.0), axis=0, keepdims=True)
        total = jnp.broadcast_to(total, gates.shape).T[:, 0:1]
        for h in range(n_piece):
            cols = rows_at(first[h] * half, half)
            acc = total * bias_ref[:, cols]
            for q in range(n_src):
                for e in range(n_loc):
                    w = w_refs[q * n_piece + h][e]
                    acc = acc + jnp.dot(left[q * n_loc + e], w, preferred_element_type=F32)
            out_ref[:, cols] = acc

    return call(
        body,
        [ids_t, bias, gates_t, *hids, *flat_w],
        [((rows, feats), F32), ((later * n_loc, rows, rank), BF16)],
        [pltpu.VMEM((rows, wide), BF16), pltpu.VMEM((n_src * n_loc, rows, rank), BF16)],
    )


def close(x, sums, lefts, wides, piece, so_far, pair):
    rows, feats = sums[0].shape
    block = rows * len(sums)
    n_loc, _, half = wides[0].shape
    n = len(sums)
    n_w = len(wides)
    n_first = 0 if so_far is None else 1

    def body(place_ref, *refs):
        refs = refs[n_first:]
        x_ref, s_refs, l_refs = refs[0], refs[1 : n + 1], refs[n + 1 : 2 * n + 1]
        w_refs = refs[2 * n + 1 : 2 * n + 1 + n_w]
        out_ref, buf, sem = refs[2 * n + 1 + n_w :]
        first = [place_ref[0], 1 - place_ref[0]] if pair else [0]
        mine = rows_at(place_ref[1] * block, block)
        copies = []
        for c in range(2):
            cut = slice(c * half // 2, (c + 1) * half // 2)
            cols = rows_at(first[piece] * half + c * (half // 2), half // 2)
            acc = jnp.concatenate([s[:, cols] for s in s_refs], axis=0)
            for q in range(n_w):
                for e in range(n_loc):
                    left = jnp.concatenate([r[q * n_loc + e] for r in l_refs], axis=0)
                    acc = acc + jnp.dot(left, w_refs[q][e, :, cut], preferred_element_type=F32)
            xs = x_ref[mine, cols].astype(F32)
            buf[:, cut] = (xs + xs * acc).astype(BF16)
            copies.append(pltpu.make_async_copy(buf.at[:, cut], out_ref.at[:, cols], sem.at[c]))
            copies[-1].start()
        for c in copies:
            c.wait()

    args = ([] if so_far is None else [so_far]) + [x, *sums, *lefts, *wides]
    return call(
        body,
        args,
        [((block, feats), BF16)],
        [pltpu.VMEM((block, half), BF16), pltpu.SemaphoreType.DMA((2,))],
        held=("out",) if so_far is None else ("out", 0),
        alias=None if so_far is None else 0,
    )[0]


def add_up(sums, lefts, wides, first, piece, x=None):
    rows = sums[0].shape[0]
    block = rows * len(sums)
    n_loc, _, half = wides[0].shape
    n, n_w = len(sums), len(wides)

    def body(place_ref, *refs):
        if x is not None:
            x_ref, *refs = refs
        s_refs, l_refs, w_refs, out_ref = refs[:n], refs[n : 2 * n], refs[2 * n : -1], refs[-1]
        at = [place_ref[0], 1 - place_ref[0]][piece] * half
        cols = rows_at(at, half)
        acc = jnp.concatenate([s[:, cols] for s in s_refs], axis=0)
        for q in range(n_w):
            for e in range(n_loc):
                left = jnp.concatenate([r[(first + q) * n_loc + e] for r in l_refs], axis=0)
                acc = acc + jnp.dot(left, w_refs[q][e], preferred_element_type=F32)
        if x is None:
            out_ref[...] = acc
        else:
            xs = x_ref[rows_at(place_ref[1] * block, block), cols].astype(F32)
            out_ref[...] = (xs + xs * acc).astype(BF16)

    kind = F32 if x is None else BF16
    args = ([] if x is None else [x]) + [*sums, *lefts, *wides]
    return call(body, args, [((block, half), kind)])[0]


def finish(x, own, acc, lefts, wide, first):
    block, half = own.shape
    n_loc = wide.shape[0]
    cut = half // 2

    def body(place_ref, x_ref, own_ref, acc_ref, *refs):
        l_refs, (w_ref, out_ref, buf, sems) = refs[:-4], refs[-4:]
        here, there = place_ref[0] * half, (1 - place_ref[0]) * half
        mine = rows_at(place_ref[1] * block, block)
        copies = [pltpu.make_async_copy(own_ref, out_ref.at[:, rows_at(here, half)], sems.at[2])]
        copies[0].start()
        for c in range(2):
            part = slice(c * cut, (c + 1) * cut)
            acc = acc_ref[:, part]
            for e in range(n_loc):
                left = jnp.concatenate([r[first * n_loc + e] for r in l_refs], axis=0)
                acc = acc + jnp.dot(left, w_ref[e, :, part], preferred_element_type=F32)
            cols = rows_at(there + c * cut, cut)
            xs = x_ref[mine, cols].astype(F32)
            buf[:, part] = (xs + xs * acc).astype(BF16)
            copies.append(pltpu.make_async_copy(buf.at[:, part], out_ref.at[:, cols], sems.at[c]))
            copies[-1].start()
        for c in copies:
            c.wait()

    return call(
        body,
        [x, own, acc, *lefts, wide],
        [((block, 2 * half), BF16)],
        [pltpu.VMEM((block, half), BF16), pltpu.SemaphoreType.DMA((3,))],
        held=("out",),
    )[0]


def relays(ne):
    return ne == 4


def relayed_by(m, n_loc):
    return [e for e in range(n_loc) if e % 2 == m - 1]


def on_device(
    nb, ne, nz, inputs, expert_ids, gate_weight, reduce_weight, middle_weight, expand_weight, bias
):
    tok, _ = inputs.shape
    n_loc = reduce_weight.shape[0]
    block = tok // ne
    n_row = block // SPLIT
    pair = nb == 2
    ids_t = expert_ids.T

    def swap(w):
        return lax.ppermute(w, "batch", [(0, 1), (1, 0)])

    def whole(w):
        return lax.all_gather(w, "batch", axis=1, tiled=True)

    if pair:
        pieces = [reduce_weight, swap(reduce_weight)]
    else:
        pieces = [whole(reduce_weight)]
        middle_weight, expand_weight = whole(middle_weight), whole(expand_weight)
    far = list(range(1, ne))
    begun = begin()
    gate_t = gate_weight.T
    near = far[:-1] if relays(ne) else far
    mids = [middle_weight] + [send(middle_weight, "expert", m, ne) for m in near]
    own, parts, logits = [], [], []
    for h in range(SPLIT):
        last = h == SPLIT - 1 and relays(ne)
        logit, mine, *sent = project(
            inputs, pieces, gate_t, begun, h, n_row, ne, pair,
            [(m, mids[ne - 1 - m]) for m in near] if last else (),
        )
        own.append(mine)
        logits.append(logit)
        parts.append([send(s, "expert", m, ne) for s, m in zip(sent, far)])
    wide = widen(expand_weight)
    wides = [wide] + [send(wide, "expert", m, ne) for m in far]
    mids = [turn(mids, parts[-1][: len(near)] if relays(ne) else [], n_row)]
    if pair:
        mids.append(swap(mids[0]))

    sums = []
    for h in range(SPLIT):
        packed = pack(
            ids_t, [own[h]] + parts[h], h, ne, nz, n_loc, logits if h == 0 else ()
        )
        sums.append([packed[0]] + [send(packed[m], "dim", m, nz) for m in range(1, nz)])
    hids, gates_t = [], None
    for h in range(SPLIT):
        hid, *made = mix(ids_t, gates_t, sums[h], mids, h, block, ne, nz, pair)
        gates_t = made[0] if made else gates_t
        hids.append([hid] + [send(hid, "dim", m, nz) for m in range(1, nz)])
    wides = [[w] + ([swap(w)] if pair else []) for w in wides]
    n_src = (ne + 1) // 2
    sums, lefts = [], []
    for h in range(SPLIT):
        total, left = expand(
            inputs, ids_t, bias[None, :], gates_t, hids[h], wides[:n_src], h, ne, nz, n_loc, pair
        )
        sums.append(total)
        lefts.append(left)
    later = wides[n_src:]
    if not pair:
        return close(inputs, sums, lefts, [w[0] for w in later], 0, None, pair)
    near_cols = add_up(sums, lefts, [w[0] for w in later], 0, 0, inputs)
    acc = add_up(sums, lefts, [w[1] for w in later[:-1]], 0, 1)
    return finish(inputs, near_cols, acc, lefts, later[-1][1], len(later) - 1)


def solution(mesh):
    sizes = dict(mesh.shape)
    in_specs = (
        P("batch", "dim"),
        P("batch", None),
        P("dim", None),
        P("expert", ("dim", "batch"), None),
        P("expert", "batch", None),
        P("expert", ("dim", "batch"), None),
        P("dim"),
    )
    out_specs = P(("batch", "expert"), "dim")
    nb, ne, nz = sizes["batch"], sizes["expert"], sizes["dim"]

    def body(*args):
        return on_device(nb, ne, nz, *args)

    return jax.shard_map(body, mesh=mesh, in_specs=in_specs, out_specs=out_specs, check_vma=False)
```

```python
import jax
import jax.numpy as jnp
from jax import lax
from jax.experimental import pallas as pl
from jax.experimental.pallas import tpu as pltpu
from jax.sharding import PartitionSpec as P


F32 = jnp.float32
BF16 = jnp.bfloat16
LAST = (((1,), (1,)), ((), ()))
MIB = 1 << 20
LANES = 128
SPLIT = 2


def peer_to(i, m, n):
    return i ^ m if n & (n - 1) == 0 else (i + m) % n


def peer_from(i, m, n):
    return i ^ m if n & (n - 1) == 0 else (i - m + n) % n


def send(x, axis, m, n):
    return lax.ppermute(x, axis, [(i, peer_to(i, m, n)) for i in range(n)])


def vmem():
    return pl.BlockSpec(memory_space=pltpu.VMEM)


def call(body, args, outs, scratch=(), limit=12, flops=None, held=(), alias=None):
    space = lambda k: pl.BlockSpec(memory_space=pl.ANY) if k in held else vmem()
    cost = None if flops is None else pl.CostEstimate(flops, 0, flops // 500)

    def placed(*refs):
        body([lax.axis_index(a) for a in ("batch", "expert", "dim")], *refs)

    return pl.pallas_call(
        placed,
        in_specs=[space(k) for k in range(len(args))],
        out_specs=[space("out") for _ in outs],
        out_shape=[jax.ShapeDtypeStruct(s, t) for s, t in outs],
        scratch_shapes=list(scratch),
        input_output_aliases={} if alias is None else {alias: 0},
        cost_estimate=cost,
        compiler_params=pltpu.CompilerParams(vmem_limit_bytes=limit * MIB),
    )(*args)


def rows_at(start, size):
    return pl.ds(pl.multiple_of(start, size), size)


def as_rows(cols_t):
    top, n = cols_t.shape
    pad = jnp.zeros((8 - top, n), cols_t.dtype)
    return jnp.concatenate([cols_t, pad], axis=0).T


def begin():
    def body(place_ref, out_ref):
        out_ref[...] = jnp.zeros(out_ref.shape, jnp.int32)

    return call(body, [], [((8, 128), jnp.int32)], flops=6_000_000_000)[0]


def project(x, pieces, gate_t, begun, h, n_row, n_expert, pair, relayed=()):
    n_loc, width, rank = pieces[0].shape
    n_piece = len(pieces)
    n_relay = len(relayed)
    more = {m: mid.shape[1] // n_loc for m, mid in relayed}
    block = n_row * SPLIT

    def body(place_ref, x_ref, *refs):
        w_refs, g_ref = refs[:n_piece], refs[n_piece]
        mid_refs = refs[n_piece + 2 : n_piece + 2 + n_relay]
        logit_ref, *outs = refs[n_piece + 2 + n_relay :]
        for (m, _), mid_ref in zip(relayed, mid_refs):
            for k, e in enumerate(relayed_by(m, n_loc)):
                at = n_row + k * more[m]
                for c in range(n_loc):
                    outs[m][at : at + more[m], c * rank : (c + 1) * rank] = mid_ref[
                        e, c * more[m] : (c + 1) * more[m], :
                    ]
        first = [place_ref[0], 1 - place_ref[0]] if pair else [0]
        starts = [
            peer_to(place_ref[1], m, n_expert) * block + h * n_row for m in range(n_expert)
        ]
        xs = []
        for p in range(n_piece):
            cols = rows_at(first[p] * width, width)
            xs.append(jnp.concatenate([x_ref[rows_at(s, n_row), cols] for s in starts], axis=0))
        for e in range(n_loc):
            acc = jnp.dot(xs[0], w_refs[0][e], preferred_element_type=F32)
            for p in range(1, n_piece):
                acc = acc + jnp.dot(xs[p], w_refs[p][e], preferred_element_type=F32)
            acc = acc.astype(BF16)
            for m in range(n_expert):
                outs[m][:n_row, e * rank : (e + 1) * rank] = acc[m * n_row : (m + 1) * n_row]
        logit = None
        for p in range(n_piece):
            gate = g_ref[:, rows_at(first[p] * width, width)]
            part = lax.dot_general(gate, xs[p][:n_row], LAST, preferred_element_type=F32)
            logit = part if logit is None else logit + part
        logit_ref[...] = logit

    return call(
        body,
        [x, *pieces, gate_t, begun] + [mid for _, mid in relayed],
        [((gate_t.shape[0], n_row), F32)]
        + [
            ((n_row + more.get(m, 0) * len(relayed_by(m, n_loc)), n_loc * rank), BF16)
            for m in range(n_expert)
        ],
        flops=3_000_000_000,
    )


def widen(wide):
    n_loc, half, rank = wide.shape

    def body(place_ref, w_ref, out_ref):
        for e in range(n_loc):
            out_ref[e] = w_ref[e].T

    return call(body, [wide], [((n_loc, rank, half), BF16)])[0]


def turn(mids, relayed, n_row):
    n_loc, half, rank = mids[0].shape
    n = len(mids)
    more = half // n_loc

    def body(place_ref, *refs):
        out_ref = refs[-1]
        for q in range(n):
            for e in range(n_loc):
                out_ref[q * n_loc + e] = refs[q][e].T
        for m in range(1, len(relayed) + 1):
            part = refs[n + m - 1]
            for k, e in enumerate(relayed_by(m, n_loc)):
                at = n_row + k * more
                rows = [part[at : at + more, c * rank : (c + 1) * rank] for c in range(n_loc)]
                out_ref[n * n_loc + e] = jnp.concatenate(rows, axis=0).T

    count = n * n_loc + (n_loc if relayed else 0)
    return call(body, [*mids, *relayed], [((count, rank, half), BF16)])[0]


def wide_ids(ids_ref, start, n, width):
    ids = as_rows(ids_ref[:, rows_at(start, n)].astype(F32))
    top = ids_ref.shape[0]
    return [jnp.broadcast_to(ids[:, j : j + 1], (n, width)).astype(BF16) for j in range(top)]


def pack(ids_t, parts, at, n_expert, n_dim, n_loc, logits=()):
    rows, wide = parts[0].shape
    rank = wide // n_loc
    per = rows // n_dim
    top = ids_t.shape[0]
    n_part = len(parts)
    n_log = len(logits)
    high_at = sum(l.shape[1] for l in logits)
    deep = logits[0].shape[0] if logits else 0
    more = -(-2 * high_at * deep // (per * LANES)) * LANES

    def body(place_ref, ids_ref, *refs):
        p_refs, scratch = refs[:n_part], refs[-1]
        l_refs, outs = refs[n_part : n_part + n_log], refs[n_part + n_log : -1]
        x_at, z_at = place_ref[1], place_ref[2]
        ids = wide_ids(ids_ref, x_at * (rows * SPLIT) + at * rows, rows, rank)
        for j in range(top):
            acc = jnp.zeros((rows, rank), BF16)
            for q in range(n_part):
                base = peer_from(x_at, q, n_expert) * n_loc
                for e in range(n_loc):
                    number = (base + e).astype(F32).astype(BF16)
                    acc = jnp.where(
                        ids[j] == number, p_refs[q][:rows, e * rank : (e + 1) * rank], acc
                    )
            scratch[:, j * rank : (j + 1) * rank] = acc
        for m in range(n_dim):
            outs[m][:, : top * rank] = scratch[rows_at(peer_to(z_at, m, n_dim) * per, per), :]
        if logits:
            full = jnp.concatenate([r[...] for r in l_refs], axis=1)
            n = full.shape[1]
            high = full.astype(BF16)
            low = (full - high.astype(F32)).astype(BF16)
            both = jnp.concatenate([high, low], axis=1)
            for m in range(n_dim):
                outs[m][:, top * rank :] = jnp.zeros((per, more), BF16)
                for k, col in enumerate(range(0, 2 * n, LANES)):
                    row, lane = k * deep % per, top * rank + k * deep // per * LANES
                    outs[m][row : row + deep, lane : lane + LANES] = both[:, col : col + LANES]

    return call(
        body,
        [ids_t, *parts, *logits],
        [((per, top * rank + more), BF16)] * n_dim,
        [pltpu.VMEM((rows, top * rank), BF16)],
    )


def mix(ids_t, gates_t, parts, mids, at, block, n_expert, n_dim, pair):
    top, _ = ids_t.shape
    rank = mids[0].shape[1]
    wide = top * rank
    per = block // SPLIT // n_dim
    n_part = len(parts)
    n_piece = len(mids)
    n_all, _, half = mids[0].shape
    n_loc = n_all // n_expert
    make = gates_t is None

    def body(place_ref, ids_ref, *refs):
        if make:
            p_refs, refs = refs[:n_part], refs[n_part:]
        else:
            g_ref, p_refs, refs = refs[0], refs[1 : n_part + 1], refs[n_part + 1 :]
        m_refs, refs = refs[:n_piece], refs[n_piece:]
        if make:
            out_ref, g_out, squash, ids_s, gate_s = refs
            logit = jnp.zeros((n_all, block), F32)
            for p in range(n_part):
                found = []
                for k in range(2 * block // LANES):
                    row, lane = k * n_all % per, wide + k * n_all // per * LANES
                    found.append(p_refs[p][row : row + n_all, lane : lane + LANES].astype(F32))
                found = jnp.concatenate(found, axis=1)
                logit = logit + found[:, :block] + found[:, block:]
            gates_t = jax.nn.sigmoid(logit)
            g_out[...] = gates_t
        else:
            out_ref, squash, ids_s, gate_s = refs
            gates_t = g_ref[...]
        x_at, z_at = place_ref[1], place_ref[2]
        first = [place_ref[0], 1 - place_ref[0]] if pair else [0]
        ids_s[...] = as_rows(ids_ref[:, rows_at(x_at * block, block)])
        gate_s[...] = gates_t.T
        mine = rows_at(at * per * n_dim + z_at * per, per)
        ids, gates = ids_s[mine, :], gate_s[mine, :]
        lane = lax.broadcasted_iota(jnp.int32, gates.shape, 1)
        chosen, gate = [], []
        for j in range(top):
            cols = slice(j * rank, (j + 1) * rank)
            acc = p_refs[0][:per, cols].astype(F32)
            for p in range(1, n_part):
                acc = acc + p_refs[p][:per, cols].astype(F32)
            squash[j * per : (j + 1) * per, :] = jnp.tanh(acc).astype(BF16)
            own = ids[:, j : j + 1]
            chosen.append(own)
            gate.append(jnp.sum(jnp.where(lane == own, gates, 0.0), axis=1, keepdims=True))
        chosen = jnp.broadcast_to(jnp.concatenate(chosen, axis=0), (top * per, half))
        sq = squash[...]
        for h in range(n_piece):
            acc = jnp.zeros((top * per, half), F32)
            for q in range(n_expert):
                base = peer_from(x_at, q, n_expert) * n_loc
                for e in range(n_loc):
                    got = jnp.dot(sq, m_refs[h][q * n_loc + e], preferred_element_type=F32)
                    acc = jnp.where(chosen == base + e, got, acc)
            hid = jnp.tanh(acc)
            for j in range(top):
                start = pl.multiple_of(j * rank + first[h] * half, half)
                gated = hid[j * per : (j + 1) * per, :] * gate[j]
                out_ref[:, pl.ds(start, half)] = gated.astype(BF16)

    return call(
        body,
        [ids_t] + ([] if make else [gates_t]) + [*parts, *mids],
        [((per, wide), BF16)] + ([((n_all, block), F32)] if make else []),
        [
            pltpu.VMEM((top * per, rank), BF16),
            pltpu.VMEM((block, 8), jnp.int32),
            pltpu.VMEM((block, n_all), F32),
        ],
    )


def expand(x, ids_t, bias, gates_t, hids, wides, at, n_expert, n_dim, n_loc, pair):
    per, wide = hids[0].shape
    top, _ = ids_t.shape
    rank = wide // top
    rows = per * n_dim
    block = rows * SPLIT
    feats = x.shape[1]
    n_src = len(wides)
    n_piece = len(wides[0])
    half = wides[0][0].shape[2]
    flat_w = [w for src in wides for w in src]
    n_h, n_w = len(hids), len(flat_w)
    later = n_expert - n_src

    def body(place_ref, ids_ref, bias_ref, g_ref, *refs):
        h_refs, w_refs = refs[:n_h], refs[n_h : n_h + n_w]
        out_ref, later_ref, hid, left = refs[n_h + n_w :]
        x_at, z_at = place_ref[1], place_ref[2]
        first = [place_ref[0], 1 - place_ref[0]] if pair else [0]
        for m in range(n_dim):
            hid[rows_at(peer_from(z_at, m, n_dim) * per, per), :] = h_refs[m][...]
        ids = wide_ids(ids_ref, x_at * block + at * rows, rows, rank)
        for q in range(n_expert):
            base = peer_from(x_at, q, n_expert) * n_loc
            for e in range(n_loc):
                number = (base + e).astype(F32).astype(BF16)
                acc = jnp.zeros((rows, rank), BF16)
                for j in range(top):
                    acc = jnp.where(ids[j] == number, hid[:, j * rank : (j + 1) * rank], acc)
                if q < n_src:
                    left[q * n_loc + e] = acc
                else:
                    later_ref[(q - n_src) * n_loc + e] = acc
        own = ids_ref[:, rows_at(x_at * block + at * rows, rows)]
        gates = g_ref[:, at * rows : (at + 1) * rows]
        number = lax.broadcasted_iota(jnp.int32, gates.shape, 0)
        hit = own[0:1, :] == number
        for j in range(1, top):
            hit = hit | (own[j : j + 1, :] == number)
        total = jnp.sum(jnp.where(hit, gates, 0.0), axis=0, keepdims=True)
        total = jnp.broadcast_to(total, gates.shape).T[:, 0:1]
        for h in range(n_piece):
            cols = rows_at(first[h] * half, half)
            acc = total * bias_ref[:, cols]
            for q in range(n_src):
                for e in range(n_loc):
                    w = w_refs[q * n_piece + h][e]
                    acc = acc + jnp.dot(left[q * n_loc + e], w, preferred_element_type=F32)
            out_ref[:, cols] = acc

    return call(
        body,
        [ids_t, bias, gates_t, *hids, *flat_w],
        [((rows, feats), F32), ((later * n_loc, rows, rank), BF16)],
        [pltpu.VMEM((rows, wide), BF16), pltpu.VMEM((n_src * n_loc, rows, rank), BF16)],
    )


def close(x, sums, lefts, wides, piece, so_far, pair):
    rows, feats = sums[0].shape
    block = rows * len(sums)
    n_loc, _, half = wides[0].shape
    n = len(sums)
    n_w = len(wides)
    n_first = 0 if so_far is None else 1

    def body(place_ref, *refs):
        refs = refs[n_first:]
        x_ref, s_refs, l_refs = refs[0], refs[1 : n + 1], refs[n + 1 : 2 * n + 1]
        w_refs = refs[2 * n + 1 : 2 * n + 1 + n_w]
        out_ref, buf, sem = refs[2 * n + 1 + n_w :]
        first = [place_ref[0], 1 - place_ref[0]] if pair else [0]
        mine = rows_at(place_ref[1] * block, block)
        copies = []
        for c in range(2):
            cut = slice(c * half // 2, (c + 1) * half // 2)
            cols = rows_at(first[piece] * half + c * (half // 2), half // 2)
            acc = jnp.concatenate([s[:, cols] for s in s_refs], axis=0)
            for q in range(n_w):
                for e in range(n_loc):
                    left = jnp.concatenate([r[q * n_loc + e] for r in l_refs], axis=0)
                    acc = acc + jnp.dot(left, w_refs[q][e, :, cut], preferred_element_type=F32)
            xs = x_ref[mine, cols].astype(F32)
            buf[:, cut] = (xs + xs * acc).astype(BF16)
            copies.append(pltpu.make_async_copy(buf.at[:, cut], out_ref.at[:, cols], sem.at[c]))
            copies[-1].start()
        for c in copies:
            c.wait()

    args = ([] if so_far is None else [so_far]) + [x, *sums, *lefts, *wides]
    return call(
        body,
        args,
        [((block, feats), BF16)],
        [pltpu.VMEM((block, half), BF16), pltpu.SemaphoreType.DMA((2,))],
        held=("out",) if so_far is None else ("out", 0),
        alias=None if so_far is None else 0,
    )[0]


def add_up(sums, lefts, wides, first, piece, x=None):
    rows = sums[0].shape[0]
    block = rows * len(sums)
    n_loc, _, half = wides[0].shape
    n, n_w = len(sums), len(wides)

    def body(place_ref, *refs):
        if x is not None:
            x_ref, *refs = refs
        s_refs, l_refs, w_refs, out_ref = refs[:n], refs[n : 2 * n], refs[2 * n : -1], refs[-1]
        at = [place_ref[0], 1 - place_ref[0]][piece] * half
        cols = rows_at(at, half)
        acc = jnp.concatenate([s[:, cols] for s in s_refs], axis=0)
        for q in range(n_w):
            for e in range(n_loc):
                left = jnp.concatenate([r[(first + q) * n_loc + e] for r in l_refs], axis=0)
                acc = acc + jnp.dot(left, w_refs[q][e], preferred_element_type=F32)
        if x is None:
            out_ref[...] = acc
        else:
            xs = x_ref[rows_at(place_ref[1] * block, block), cols].astype(F32)
            out_ref[...] = (xs + xs * acc).astype(BF16)

    kind = F32 if x is None else BF16
    args = ([] if x is None else [x]) + [*sums, *lefts, *wides]
    return call(body, args, [((block, half), kind)])[0]


def finish(x, own, acc, lefts, wide, first):
    block, half = own.shape
    n_loc = wide.shape[0]
    cuts = ((0, half // 2), (half // 2, half // 4), (3 * half // 4, half // 4))

    def body(place_ref, x_ref, own_ref, acc_ref, *refs):
        l_refs, (w_ref, out_ref, buf, sems) = refs[:-4], refs[-4:]
        here, there = place_ref[0] * half, (1 - place_ref[0]) * half
        mine = rows_at(place_ref[1] * block, block)
        copies = [pltpu.make_async_copy(own_ref, out_ref.at[:, rows_at(here, half)], sems.at[3])]
        copies[0].start()
        for c, (at, cut) in enumerate(cuts):
            part = slice(at, at + cut)
            acc = acc_ref[:, part]
            for e in range(n_loc):
                left = jnp.concatenate([r[first * n_loc + e] for r in l_refs], axis=0)
                acc = acc + jnp.dot(left, w_ref[e, :, part], preferred_element_type=F32)
            cols = rows_at(there + at, cut)
            xs = x_ref[mine, cols].astype(F32)
            buf[:, part] = (xs + xs * acc).astype(BF16)
            copies.append(pltpu.make_async_copy(buf.at[:, part], out_ref.at[:, cols], sems.at[c]))
            copies[-1].start()
        for c in copies:
            c.wait()

    return call(
        body,
        [x, own, acc, *lefts, wide],
        [((block, 2 * half), BF16)],
        [pltpu.VMEM((block, half), BF16), pltpu.SemaphoreType.DMA((4,))],
        held=("out",),
    )[0]


def relays(ne):
    return ne == 4


def relayed_by(m, n_loc):
    return [e for e in range(n_loc) if e % 2 == m - 1]


def on_device(
    nb, ne, nz, inputs, expert_ids, gate_weight, reduce_weight, middle_weight, expand_weight, bias
):
    tok, _ = inputs.shape
    n_loc = reduce_weight.shape[0]
    block = tok // ne
    n_row = block // SPLIT
    pair = nb == 2
    ids_t = expert_ids.T

    def swap(w):
        return lax.ppermute(w, "batch", [(0, 1), (1, 0)])

    def whole(w):
        return lax.all_gather(w, "batch", axis=1, tiled=True)

    if pair:
        pieces = [reduce_weight, swap(reduce_weight)]
    else:
        pieces = [whole(reduce_weight)]
        middle_weight, expand_weight = whole(middle_weight), whole(expand_weight)
    far = list(range(1, ne))
    begun = begin()
    gate_t = gate_weight.T
    near = far[:-1] if relays(ne) else far
    mids = [middle_weight] + [send(middle_weight, "expert", m, ne) for m in near]
    own, parts, logits = [], [], []
    for h in range(SPLIT):
        last = h == SPLIT - 1 and relays(ne)
        logit, mine, *sent = project(
            inputs, pieces, gate_t, begun, h, n_row, ne, pair,
            [(m, mids[ne - 1 - m]) for m in near] if last else (),
        )
        own.append(mine)
        logits.append(logit)
        parts.append([send(s, "expert", m, ne) for s, m in zip(sent, far)])
    wide = widen(expand_weight)
    wides = [wide] + [send(wide, "expert", m, ne) for m in far]
    mids = [turn(mids, parts[-1][: len(near)] if relays(ne) else [], n_row)]
    if pair:
        mids.append(swap(mids[0]))

    sums = []
    for h in range(SPLIT):
        packed = pack(
            ids_t, [own[h]] + parts[h], h, ne, nz, n_loc, logits if h == 0 else ()
        )
        sums.append([packed[0]] + [send(packed[m], "dim", m, nz) for m in range(1, nz)])
    hids, gates_t = [], None
    for h in range(SPLIT):
        hid, *made = mix(ids_t, gates_t, sums[h], mids, h, block, ne, nz, pair)
        gates_t = made[0] if made else gates_t
        hids.append([hid] + [send(hid, "dim", m, nz) for m in range(1, nz)])
    wides = [[w] + ([swap(w)] if pair else []) for w in wides]
    n_src = (ne + 1) // 2
    sums, lefts = [], []
    for h in range(SPLIT):
        total, left = expand(
            inputs, ids_t, bias[None, :], gates_t, hids[h], wides[:n_src], h, ne, nz, n_loc, pair
        )
        sums.append(total)
        lefts.append(left)
    later = wides[n_src:]
    if not pair:
        return close(inputs, sums, lefts, [w[0] for w in later], 0, None, pair)
    near_cols = add_up(sums, lefts, [w[0] for w in later], 0, 0, inputs)
    acc = add_up(sums, lefts, [w[1] for w in later[:-1]], 0, 1)
    return finish(inputs, near_cols, acc, lefts, later[-1][1], len(later) - 1)


def solution(mesh):
    sizes = dict(mesh.shape)
    in_specs = (
        P("batch", "dim"),
        P("batch", None),
        P("dim", None),
        P("expert", ("dim", "batch"), None),
        P("expert", "batch", None),
        P("expert", ("dim", "batch"), None),
        P("dim"),
    )
    out_specs = P(("batch", "expert"), "dim")
    nb, ne, nz = sizes["batch"], sizes["expert"], sizes["dim"]

    def body(*args):
        return on_device(nb, ne, nz, *args)

    return jax.shard_map(body, mesh=mesh, in_specs=in_specs, out_specs=out_specs, check_vma=False)
```
